32 devices in a mesh: flow: 8 (over y, x, core), span: 4 (over z).
Axes of the slice: x: 2, y: 2, z: 4, core: 2. Of those that a mesh axis runs over, the one named last changes fastest.
Arguments:
- solid_start: float32 [32, 512, 512], P(None, 'flow', 'span'), may hold values from -6 to 6
- heat_gen: float32 [32, 512, 512], P(None, 'flow', 'span'), may hold values from 0 to 0.05
- conductance: float32 [64, 16384], P('span', 'flow'), may hold values from 0 to 1, as said below
- heat_capacity: float32 [64], P('span'), may hold values from 0.2 to 1
- inlet_temp: float32 [64], P('span'), may hold values from -4 to 4
- wall_owner: int32 [8192, 1], P(('flow', 'span')), may hold values from 0 to 7; in each aligned block of 256 rows (0 to 255, 256 to 511, ...) at most 64 rows name the same one
- wall_row: int32 [8192, 1], P(('flow', 'span')), may hold values from 0 to 63
Outputs:
- solid_final: float32 [32, 512, 512], P(None, 'flow', 'span')
- coolant_final: float32 [64, 16384], P('span', 'flow')
The draws below stay inside these ranges and needn't reach their ends.
Inputs may be any that keep to these rules, and one draw needn't show every extreme that they name: `conductance`: Positive. `wall_owner`: within the segments of one device (aligned blocks of 256 rows) no flow index is named more than 64 times, and some flow index is named exactly 64 times.
All inputs are finite; a program needn't handle non-finite values.
Results may differ from the reference program's by a relative error of at most 0.0003.
Values sent between devices are 32-bit elements; how exact they have to be, the bound alone decides.
A program may use at most 128 MiB of HBM per device.

```python
import math
import jax
import jax.numpy as jnp
import numpy as np
from jax import lax

SEG = 128
NZ = 32
CX = 64
CH_DEV = 16
ST_DEV = 2048
STEPS = 10
NX = 512
NY = 512
CHANNELS = 64
CHANNEL_STATIONS = 16384
SEG_DEV = 256
SEGS = 8192
CAP = 64
N_FLOW = 8
N_SPAN = 4


def draw_conductance(key, part):
    random_child_keys = jax.random.split(key, 6)
    solid_grid_shape = (CHANNELS, CHANNEL_STATIONS)
    fast_share = 0.5
    fast_mask = jax.random.uniform(random_child_keys[0], (CHANNELS, 1)) < fast_share
    slow_rates = jnp.exp(jax.random.uniform(random_child_keys[1], (CHANNELS, 1), jnp.float32, math.log(5.0), math.log(40.0))) / CHANNEL_STATIONS
    fast_rates = jnp.exp(jax.random.uniform(random_child_keys[2], (CHANNELS, 1), jnp.float32, math.log(1.0 / 50.0), math.log(1.0 / 30.0)))
    decay_rates = jnp.where(fast_mask, fast_rates, slow_rates)
    surface_texture = jax.random.uniform(random_child_keys[3], solid_grid_shape, jnp.float32, 0.5, 1.5)
    surge_event_mask = jax.random.uniform(random_child_keys[4], solid_grid_shape) < 3.0 / CHANNEL_STATIONS
    surge_heat_loss = jax.random.uniform(random_child_keys[5], solid_grid_shape, jnp.float32, 0.2, 0.5)
    sampled_values = jnp.where(surge_event_mask, -jnp.log(1.0 - surge_heat_loss), decay_rates * surface_texture)
    return sampled_values.astype(jnp.float32)


def set_ends(array, rng, low, largest):
    shape = array.shape
    place = [jax.random.randint(jax.random.fold_in(rng, axis), (), 0, shape[axis]) for axis in range(len(shape))]
    array = array.at[tuple(place)].set(low)
    longest = shape.index(max(shape))
    place[longest] = (place[longest] + 1) % shape[longest]
    return array.at[tuple(place)].set(largest)


def block_scale(own_key, extent, cuts, least, top_value):
    gain, own = 1.0, jax.random.fold_in(own_key, 6)
    for axis_at, shards_of in cuts:
        heights = jnp.exp(jax.random.uniform(jax.random.fold_in(own, axis_at), (shards_of,), jnp.float32, least / len(cuts), top_value / len(cuts)))
        gain = gain * jnp.repeat(heights, extent[axis_at] // shards_of).reshape([-1 if axis == axis_at else 1 for axis in range(len(extent))])
    return gain


def deal_out(own_key, own, number, rows, amount, top, reach, skew):
    sequence = jax.random.permutation(own_key, amount)
    crowded, common = portions_of(amount, rows * top, reach, skew, True), portions_of(amount, rows * top, reach, skew, False)
    places = jnp.arange(amount)

    def named(sizes, rotation):
        used = int((sizes > 0).sum())
        fixed = max(1, used // 4)
        shifted = fixed + (places - fixed + rotation * (used - fixed)) % max(1, amount - fixed)
        return jnp.zeros((amount,), jnp.int32).at[sequence[jnp.where(places < fixed, places, shifted)]].set(jnp.asarray(sizes, jnp.int32))

    sizes = jnp.where(number % 4 == 0, named(crowded, number // 4), named(common, number - number // 4 - 1))
    mixed = jax.random.permutation(jax.random.fold_in(own, 3), amount)
    giver, receiver = mixed[0:amount // 2 * 2:2], mixed[1:amount // 2 * 2:2]
    margin = jnp.minimum(sizes[giver] - 1, reach - sizes[receiver]) // 2
    margin = jnp.where((giver == sequence[0]) | (receiver == sequence[0]) | (sizes[receiver] == 0), 0, jnp.maximum(margin, 0))
    shifted = jax.random.randint(jax.random.fold_in(own, 4), (amount // 2,), 0, 1 << 20) % (margin + 1)
    sizes = sizes.at[giver].add(-shifted).at[receiver].add(shifted)
    labels = jnp.searchsorted(jnp.cumsum(sizes), jnp.arange(rows * top), side="right").astype(jnp.int32)
    table = labels.reshape(top, rows).T
    table = table[jax.random.permutation(jax.random.fold_in(own, 1), rows)]
    rotation = jax.random.randint(jax.random.fold_in(own, 2), (rows, 1), 0, top)
    return jnp.take_along_axis(table, (jnp.arange(top)[None, :] + rotation) % top, axis=1)


def portions_of(count, total, most, lean, full):
    portions = [(1 << 20) // math.isqrt(grade ** lean) + 1 for grade in range(1, count + 1)]
    largest = most if full else min(most, max(-(-total // count), total * portions[0] // sum(portions)))
    least = 1 if total - largest >= count - 1 else 0
    given, rest = [largest] + [least] * (count - 1), total - largest - least * (count - 1)
    while rest > 0:
        free = [i for i in range(1, count) if given[i] < largest] or [i for i in range(1, count) if given[i] < most]
        pool, budget = sum([portions[i] for i in free]), rest
        for i in free:
            extra = min(most - given[i], max(1, budget * portions[i] // pool), rest)
            given[i] = given[i] + extra
            rest = rest - extra
    return np.array(given)


def noise(own_key, dims, scale, most, shards=(), kind=jnp.bfloat16):
    level = block_scale(own_key, dims, shards, -0.22, 0.18) if shards else 1.0
    array = jax.random.normal(own_key, dims, jnp.float32) * scale * level
    return jnp.minimum(jnp.maximum(array, -most), most).astype(kind)


def setup_inputs(seed: int = 0) -> dict:
    seeds = jax.random.split(jax.random.key(seed), 8)
    solid_start = noise(seeds[0], (NZ, NX, NY), 1.0, 6.0, ((1, 8), (2, 4)), jnp.float32)
    heat_gen = jnp.clip(0.05 * jax.random.uniform(seeds[1], (NZ, NX, NY), jnp.float32) ** block_scale(seeds[1], (NZ, NX, NY), ((1, 8), (2, 4)), -0.2, 0.2), 0.0, 0.05)
    conductance = draw_conductance(jax.random.fold_in(seeds[7], 71), 0)
    heat_capacity = jnp.clip(jnp.exp(math.log(1.0) - 1.609438 * jax.random.uniform(seeds[3], (CHANNELS,), jnp.float32) ** block_scale(seeds[3], (CHANNELS,), ((0, 4),), -0.2, 0.2)), 0.2, 1.0)
    inlet_temp = noise(seeds[4], (CHANNELS,), 1.0, 4.0, ((0, 4),), jnp.float32)
    wall_owner_keys = jax.random.split(jax.random.fold_in(seeds[5], 1), SEGS // SEG_DEV)
    wall_owner_turns = jax.random.permutation(jax.random.fold_in(seeds[5], 3), SEGS // SEG_DEV)
    wall_owner = jax.vmap(lambda own, number: deal_out(jax.random.fold_in(seeds[5], 2), own, number, SEG_DEV, N_FLOW, 1, CAP, 2))(wall_owner_keys, wall_owner_turns).reshape((SEGS, 1))
    wall_row = set_ends(jax.random.randint(seeds[6], (SEGS, 1), 0, CX), jax.random.fold_in(seeds[6], 1), 0, CX - 1).astype(jnp.int32)
    return {"solid_start": solid_start, "heat_gen": heat_gen, "conductance": conductance, "heat_capacity": heat_capacity, "inlet_temp": inlet_temp, "wall_owner": wall_owner, "wall_row": wall_row}


KAPPA = 0.16


def compose(earlier, later):
    return (earlier[0] * later[0], later[0] * earlier[1] + later[1])


def regroup(sampled_values, seg_count):
    sampled_values = sampled_values.reshape(N_FLOW, N_SPAN, CH_DEV, seg_count)
    return jnp.transpose(sampled_values, (1, 2, 0, 3)).reshape(CHANNELS, N_FLOW * seg_count)


def conduct(field, heat_gen):
    padded = jnp.pad(field, 1)
    beside = padded[2:, 1:-1, 1:-1] + padded[:-2, 1:-1, 1:-1]
    beside = beside + padded[1:-1, 2:, 1:-1] + padded[1:-1, :-2, 1:-1]
    beside = beside + padded[1:-1, 1:-1, 2:] + padded[1:-1, 1:-1, :-2]
    return field + KAPPA * (beside - 6.0 * field) + heat_gen


def reference(solid_start, heat_gen, conductance, heat_capacity, inlet_temp, wall_owner, wall_row):
    seg_count = ST_DEV // SEG
    wall_cell = regroup(wall_owner[:, 0], seg_count) * CX + regroup(wall_row[:, 0], seg_count)
    wall_cell = wall_cell.astype(jnp.int32)
    span_band = (jnp.arange(CHANNELS, dtype=jnp.int32) // CH_DEV).astype(jnp.int32)[:, None]
    decays = jnp.exp(-conductance)
    solid_field = solid_start
    coolant = jnp.zeros((CHANNELS, CHANNEL_STATIONS), jnp.float32)
    for turn in range(STEPS):
        bottom_layer = solid_field[0].reshape(NX, N_SPAN, SEG)
        wall_temp = bottom_layer[wall_cell, span_band].reshape(CHANNELS, CHANNEL_STATIONS)
        gain_pre, shift_pre = lax.associative_scan(compose, (decays, (1.0 - decays) * wall_temp), axis=1)
        coolant = gain_pre * inlet_temp[:, None] + shift_pre
        upstream = jnp.concatenate([inlet_temp[:, None], coolant[:, :-1]], axis=1)
        heat_flow = heat_capacity[:, None] * (coolant - upstream)
        wall_sink = jnp.zeros((NX, N_SPAN, SEG), jnp.float32)
        wall_sink = wall_sink.at[wall_cell, span_band].add(heat_flow.reshape(CHANNELS, N_FLOW * seg_count, SEG))
        solid_field = conduct(solid_field, heat_gen)
        solid_field = solid_field.at[0].add(-wall_sink.reshape(NX, NY))
    return solid_field, coolant
```

```python
import jax
import jax.numpy as jnp
from jax import lax
from jax.experimental import pallas as pl
from jax.experimental.pallas import tpu as pltpu
from jax.sharding import PartitionSpec as P

STEPS = 10
KAPPA = 0.16
MESH = pl.DeviceIdType.MESH
F32 = jnp.float32
BF16 = jnp.bfloat16


def split(x):
    hi = x.astype(BF16)
    lo = (x - hi.astype(F32)).astype(BF16)
    return hi, lo


def kernel(dims, owner_ref, row_ref, cap_ref, inlet_ref, cond_ref, start_ref, gen_ref,
           solid_out, cool_out, s):
    flow, span, layers, block, seg, channels, count, group, keep = dims
    width = flow * channels
    cells = flow * block
    half = flow // 2
    tiles = block // 8
    lines = cells // 8
    packs = -(-lines // (seg // 2))
    me = lax.axis_index("flow")
    at = lax.axis_index("span")
    mate = me + 1 - 2 * lax.rem(me, 2)
    above, below = at > 0, at < span - 1
    before, after = me > 0, me < flow - 1

    lane = lax.broadcasted_iota(jnp.int32, (8, seg), 1)
    pair = lane // 2
    lane_b = lax.broadcasted_iota(jnp.int32, (block, seg), 1)
    row_b = lax.broadcasted_iota(jnp.int32, (block, seg), 0)
    first_b, last_b = lane_b == 0, lane_b == seg - 1
    top_b, low_b = row_b == 0, row_b == block - 1

    def remote(src, dst, send, recv, device):
        return pltpu.make_async_remote_copy(
            src_ref=src, dst_ref=dst, send_sem=send, recv_sem=recv,
            device_id=device, device_id_type=MESH)

    kinds = (
        (s.idx_own, lambda f: s.idx.at[f]),
        (start_ref.at[pl.ds(0, 2)], lambda f: s.first.at[f]),
        (cond_ref, lambda f: s.gain.at[f]),
        (gen_ref.at[0], lambda f: s.gen0.at[f]),
    )

    def direct(kind, hop):
        src, dst = kinds[kind]
        to = lax.rem(me + 2 * hop, flow)
        return remote(src, dst(me), s.once_send.at[kind, 2 * hop - 1], s.once_recv.at[kind, 2 * hop - 1], (to, at))

    def to_mate(kind):
        src, dst = kinds[kind]
        return remote(src, dst(me), s.once_send.at[kind, 0], s.once_recv.at[kind, 0], (mate, at))

    def relay(kind, hop):
        _, dst = kinds[kind]
        origin = lax.rem(me + flow - 2 * hop, flow)
        return remote(dst(origin), dst(origin), s.once_send.at[kind, 2 * hop], s.once_recv.at[kind, 2 * hop], (mate, at))

    def layer_copy(slot, hop):
        peer = lax.rem(me + hop, flow)
        return remote(s.one.at[slot, me], s.one.at[slot, me],
                      s.one_send.at[hop - 1], s.one_recv.at[slot, hop - 1], (peer, at))

    def side_copy(slot, side):
        return remote(s.side_out, s.side_in.at[slot, 1 - side],
                      s.side_send.at[side], s.side_recv.at[slot, 1 - side], (me, at - 1 + 2 * side))

    def rim_copy(slot, side):
        return remote(s.rim_out, s.rim_in.at[slot, 1 - side],
                      s.rim_send.at[side], s.rim_recv.at[slot, 1 - side], (me, at - 1 + 2 * side))

    def col_copy(slot, side):
        return remote(s.col_out, s.col_in.at[slot, 1 - side],
                      s.col_send.at[side], s.col_recv.at[slot, 1 - side], (me, at - 1 + 2 * side))

    def row_copy(slot, side):
        return remote(s.row_out.at[side], s.row_in.at[slot, 1 - side],
                      s.row_send.at[side], s.row_recv.at[slot, 1 - side], (me - 1 + 2 * side, at))

    def both(copy, pair_of, act):
        for side, there in enumerate(pair_of):
            @pl.when(there)
            def _():
                act(copy, side)

    in_span, in_flow = (above, below), (before, after)

    def start(copy, slot, pair_of):
        both(copy, pair_of, lambda c, side: c(slot, side).start())

    def sent(copy, slot, pair_of):
        both(copy, pair_of, lambda c, side: c(slot, side).wait_send())

    def arrived(copy, slot, pair_of):
        both(copy, pair_of, lambda c, side: c(slot, 1 - side).wait_recv())

    s.side_in[...] = jnp.zeros_like(s.side_in)
    s.rim_in[...] = jnp.zeros_like(s.rim_in)
    s.col_in[...] = jnp.zeros_like(s.col_in)
    s.row_in[...] = jnp.zeros_like(s.row_in)
    s.idx_own[...] = jnp.zeros_like(s.idx_own)
    per = owner_ref.shape[0]
    s.idx_own[0:per, :] = owner_ref[...].astype(F32)
    s.idx_own[per:2 * per, :] = row_ref[...].astype(F32)
    barrier = pltpu.get_barrier_semaphore()
    for hop in range(1, flow):
        pl.semaphore_signal(barrier, inc=1, device_id=(lax.rem(me + hop, flow), at), device_id_type=MESH)
    for side, there in enumerate(in_span):
        @pl.when(there)
        def _():
            pl.semaphore_signal(barrier, inc=1, device_id=(me, at - 1 + 2 * side), device_id_type=MESH)
    pl.semaphore_wait(barrier, flow - 1 + above.astype(jnp.int32) + below.astype(jnp.int32))
    for kind in range(len(kinds)):
        for hop in range(1, half):
            direct(kind, hop).start()
        to_mate(kind).start()
    s.idx[me] = s.idx_own[...]
    s.first[me] = start_ref[0:2]
    s.gain[me] = cond_ref[...]
    s.gen0[me] = gen_ref[0]

    def packed(marks, value, place):
        for r in range(tiles):
            p, k = place(r)
            turned = pltpu.roll(value[8 * r:8 * r + 8], 2 * k + 1, 1)
            marks[p] = jnp.where(pair == k, turned, marks[p])
        return marks

    def merged(low, high):
        return jnp.where(lax.rem(lane, 2) == 0, pltpu.roll(high, seg - 1, 1), pltpu.roll(low, 1, 1))

    def unpacked(marks, place):
        return jnp.concatenate(
            [pltpu.roll(marks[p], seg - 1 - 2 * k, 1) for p, k in (place(r) for r in range(tiles))], axis=0)

    def rim_place(r):
        return 0, r

    def col_place(z):
        per_pack = seg // 2 // layers
        return lambda r: (r // per_pack, z + layers * (r % per_pack))

    def side_place(b):
        return lambda r: divmod(b * tiles + r, seg // 2)

    col_packs = s.col_out.shape[0]
    empty = jnp.zeros((8, seg), F32)

    def around(c, low_row, high_row, halo):
        beside = jnp.where(top_b, low_row, pltpu.roll(c, 1, 0))
        beside = beside + jnp.where(low_b, high_row, pltpu.roll(c, block - 1, 0))
        beside = beside + jnp.where(first_b, halo, pltpu.roll(c, 1, 1))
        return beside + jnp.where(last_b, halo, pltpu.roll(c, seg - 1, 1))

    marks = [empty] * col_packs
    for side in range(2):
        s.row_out[side] = jnp.zeros_like(s.row_out[side])
    s.field[0, layers] = jnp.zeros((block, seg), F32)
    s.field[1, layers] = jnp.zeros((block, seg), F32)

    def note_rows(z, new):
        s.row_out[0, z:z + 1, :] = new[0:1, :]
        s.row_out[1, z:z + 1, :] = new[block - 1:block, :]

    new = start_ref[1]
    s.field[0, 1] = new
    s.rim_out[...] = packed([empty], new, rim_place)[0]
    start(rim_copy, 0, in_span)
    for z in range(2, layers):
        new = start_ref[z]
        s.field[0, z] = new
        note_rows(z, new)
        marks = packed(marks, new, col_place(z))
    for p in range(col_packs):
        s.col_out[p] = marks[p]
    start(row_copy, 0, in_flow)
    start(col_copy, 0, in_span)

    mid = seg // 2 - 1
    i2 = lax.rem(lax.broadcasted_iota(jnp.int32, (2 * seg, 2 * seg), 0), seg)
    j2 = lax.broadcasted_iota(jnp.int32, (2 * seg, 2 * seg), 1)
    tri = jnp.where((i2 <= j2) | (j2 >= seg), 1.0, 0.0).astype(BF16)
    s.tri[...] = tri
    i3 = lax.rem(lax.broadcasted_iota(jnp.int32, (3 * seg, 3 * seg), 0), seg)
    j3 = lax.broadcasted_iota(jnp.int32, (3 * seg, 3 * seg), 1)
    lower = jnp.where(i3 <= mid, 1.0, 0.0)
    spread = jnp.where(j3 < seg, jnp.where(i3 <= j3, 1.0, 0.0) - lower,
                       jnp.where(j3 < 2 * seg, lower, 1.0 - lower)).astype(BF16)
    eye = (lax.broadcasted_iota(jnp.int32, (channels, channels), 0)
           == lax.broadcasted_iota(jnp.int32, (channels, channels), 1))

    def column(ref):
        wide = jnp.where(eye, jnp.broadcast_to(ref[...], (channels, channels)), 0.0)
        return jnp.broadcast_to(jnp.sum(wide, axis=1, keepdims=True), (channels, seg))

    capacity, inlet = column(cap_ref), column(inlet_ref)

    def arrivals(kind, i):
        hop = i // 2
        odd = lax.rem(i, 2) == 1

        @pl.when(jnp.logical_and(jnp.logical_not(odd), i > 0))
        def _():
            direct(kind, hop).wait_recv()
            relay(kind, hop).start()

        @pl.when(i == 1)
        def _():
            to_mate(kind).wait_recv()

        @pl.when(jnp.logical_and(odd, i > 1))
        def _():
            relay(kind, hop).wait_recv()

    def gather_kind(kind):
        def body(i, carry):
            arrivals(kind, i)
            return carry
        lax.fori_loop(0, flow, body, 0)

    gather_kind(0)
    share = seg // count
    lane_i = lax.broadcasted_iota(jnp.int32, (channels, seg), 1) // count
    chan_i = lax.rem(lax.broadcasted_iota(jnp.int32, (channels, seg), 0), share)
    here = lane_i == chan_i

    def one_source(f, carry):
        def taken(base):
            rows = jnp.concatenate(
                [jnp.broadcast_to(s.idx[f, base + a:base + a + 1, :], (share, seg)) for a in range(per)], axis=0)
            return jnp.where(here, rows, 0.0).astype(BF16)
        s.seats[f] = jnp.concatenate([taken(0), taken(per)], axis=1)
        return carry

    lax.fori_loop(0, flow, one_source, 0)
    seats = s.seats[...].reshape(width, 2 * seg)
    ci = lax.broadcasted_iota(jnp.int32, (2 * seg, seg), 0)
    weight = jnp.where(ci < seg, float(block), 1.0)
    turn_of = lax.rem(ci, count)
    ri = lax.broadcasted_iota(jnp.int32, (count, 2 * seg), 1)
    rt = lax.broadcasted_iota(jnp.int32, (count, 2 * seg), 0)
    pick = jnp.where(lax.rem(ri, count) == rt, jnp.where(ri < seg, float(block), 1.0), 0.0).astype(BF16)
    s.along[...] = lax.dot_general(pick, seats, (((1,), (1,)), ((), ())), preferred_element_type=F32)

    def one_turn(t, carry):
        chosen = jnp.where(turn_of == t, weight, 0.0).astype(BF16)
        cell = jnp.dot(seats, chosen, preferred_element_type=F32)
        if keep:
            lanes = lax.broadcasted_iota(jnp.int32, (width, seg), 1).astype(F32)
            rows = pl.ds(pl.multiple_of(t * width, width), width)
            for k in range(cells // seg):
                s.take[rows, k * seg:(k + 1) * seg] = jnp.where(cell - float(k * seg) == lanes, 1.0, 0.0).astype(BF16)
        else:
            s.take[t] = cell
        return carry

    lax.fori_loop(0, count, one_turn, 0)
    if keep:
        for t in range(count):
            for b in range(flow):
                rows = lax.broadcasted_iota(jnp.int32, (block, width), 0).astype(F32) + float(b * block)
                s.give[b * block:(b + 1) * block, t * width:(t + 1) * width] = jnp.where(
                    rows == s.along[t:t + 1, :], 1.0, 0.0).astype(BF16)

    def take_rows(t0):
        if keep:
            return s.take[t0 * width:(t0 + group) * width, :]
        cell = s.take[t0:t0 + group].reshape(group * width, seg)
        lanes = lax.broadcasted_iota(jnp.int32, (group * width, seg), 1).astype(F32)
        return jnp.concatenate(
            [jnp.where(cell - float(k * seg) == lanes, 1.0, 0.0).astype(BF16) for k in range(cells // seg)], axis=1)

    def give_rows(t0, b):
        if keep:
            return s.give[b * block:(b + 1) * block, t0 * width:(t0 + group) * width]
        rows = lax.broadcasted_iota(jnp.int32, (block, width), 0).astype(F32) + float(b * block)
        return jnp.concatenate(
            [jnp.where(rows == s.along[t:t + 1, :], 1.0, 0.0).astype(BF16) for t in range(t0, t0 + group)], axis=1)

    gather_kind(1)

    def place_first(f, carry):
        s.plane[0, f] = s.first[f, 0]
        s.one[0, f] = s.first[f, 1]
        return carry

    lax.fori_loop(0, flow, place_first, 0)
    side_marks = [empty] * packs
    for b in range(flow):
        c = s.plane[0, b]
        side_marks = packed(side_marks, c, side_place(b))
        hi, lo = split(c)
        s.base[b * block:(b + 1) * block, 0:seg] = hi
        s.base[b * block:(b + 1) * block, seg:2 * seg] = lo
    for p in range(packs):
        s.side_out[p] = side_marks[p]
    start(side_copy, 0, in_span)

    def chunk(ref, t):
        return ref[:, :, t * seg:(t + 1) * seg].reshape(width, seg)

    def constants(i, carry):
        arrivals(2, i)
        hop = i // 2
        from_me = lax.rem(me + flow - 2 * hop, flow)
        from_mate = lax.rem(mate + flow - 2 * hop, flow)
        f = jnp.where(lax.rem(i, 2) == 0, from_me, from_mate)

        @pl.when(jnp.logical_and(lax.rem(i, 2) == 0, i > 0))
        def _():
            relay(2, hop).wait_send()

        k = jnp.concatenate([s.gain[f, :, t * seg:(t + 1) * seg] for t in range(count)], axis=0)
        k1 = k.astype(BF16)
        rest = k - k1.astype(F32)
        k2 = rest.astype(BF16)
        k3 = (rest - k2.astype(F32)).astype(BF16)
        sums = jnp.dot(jnp.concatenate([k1, k2, k3], axis=1), spread, preferred_element_type=F32)
        run = jnp.ones((channels, seg), F32)
        for t in range(count):
            rows = slice(t * channels, (t + 1) * channels)
            cols = slice(t * seg, (t + 1) * seg)
            kt, depth = k[rows], sums[rows, 0:seg]
            fore, rear = jnp.exp(-sums[rows, seg:2 * seg]), jnp.exp(-sums[rows, 2 * seg:])
            s.gain[f, :, cols] = (1.0 - jnp.exp(-kt)) * jnp.exp(depth)
            s.fall[f, :, cols] = jnp.exp(-depth)
            s.heat_of[f, :, cols] = (jnp.exp(kt) - 1.0) * capacity
            s.fore[f, :, cols] = fore
            s.rear[f, :, cols] = rear
            s.reach[f, :, cols] = run
            run = run * (fore * rear)
        s.whole[f] = run
        return carry

    lax.fori_loop(0, flow, constants, 0)
    gather_kind(3)

    def coolant():
        base = s.base[...]
        run = jnp.zeros((width, seg), F32)
        for t0 in range(0, count, group):
            found = jnp.dot(take_rows(t0), base, preferred_element_type=F32)
            w = found[:, :seg] + found[:, seg:]
            gains = jnp.concatenate([chunk(s.gain, t) for t in range(t0, t0 + group)], axis=0)
            hi, lo = split(gains * w)
            sums = jnp.dot(jnp.concatenate([hi, lo], axis=1), s.tri[...], preferred_element_type=F32)
            for i in range(group):
                t = t0 + i
                rows = slice(i * width, (i + 1) * width)
                s.wall[t] = w[rows]
                s.part[t] = sums[rows, :seg]
                s.run[t] = run
                run = chunk(s.rear, t) * (sums[rows, seg:] + chunk(s.fore, t) * run)
        enter = inlet
        for f in range(flow):
            s.enter[f] = enter
            enter = run[f * channels:(f + 1) * channels] + s.whole[f] * enter
        enter = s.enter[...].reshape(width, seg)
        for t0 in range(0, count, group):
            for t in range(t0, t0 + group):
                first = s.run[t] + chunk(s.reach, t) * enter
                cool = chunk(s.fall, t) * (s.part[t] + chunk(s.fore, t) * first)
                hi, lo = split(chunk(s.heat_of, t) * (s.wall[t] - cool))
                s.heat[t * width:(t + 1) * width, 0:seg] = hi
                s.heat[t * width:(t + 1) * width, seg:2 * seg] = lo

    def sinks(b):
        total = jnp.zeros((block, 2 * seg), F32)
        for t0 in range(0, count, group):
            total = total + jnp.dot(give_rows(t0, b), s.heat[t0 * width:(t0 + group) * width, :],
                                    preferred_element_type=F32)
        return total[:, :seg] + total[:, seg:]

    def step(turn, carry):
        slot, later = lax.rem(turn, 2), lax.rem(turn + 1, 2)
        held, next_held = lax.rem(turn, 4), lax.rem(turn + 1, 4)
        more = turn < STEPS - 1

        @pl.when(turn > 0)
        def _():
            layer_copy(held, 1).wait_recv()
            if flow > 2:
                layer_copy(held, flow - 1).wait_recv()
            for hop in range(1, flow):
                layer_copy(held, hop).wait_send()
        arrived(rim_copy, slot, in_span)
        sent(rim_copy, slot, in_span)
        c = s.field[slot, 1]
        low = s.one[held, jnp.maximum(me - 1, 0), block - 1:block, :]
        high = s.one[held, jnp.minimum(me + 1, flow - 1), 0:1, :]
        halo = unpacked([merged(s.rim_in[slot, 0], s.rim_in[slot, 1])], rim_place)
        beside = around(c, jnp.where(before, low, 0.0), jnp.where(after, high, 0.0), halo)
        beside = beside + s.plane[slot, me] + s.field[slot, 2]
        new = c + KAPPA * (beside - 6.0 * c) + gen_ref[1]
        s.field[later, 1] = new
        s.one[next_held, me] = new
        s.rim_out[...] = packed([empty], new, rim_place)[0]

        @pl.when(more)
        def _():
            for hop in range(1, flow):
                layer_copy(next_held, hop).start()
        @pl.when(more)
        def _():
            start(rim_copy, later, in_span)

        coolant()

        arrived(row_copy, slot, in_flow)
        sent(row_copy, slot, in_flow)
        arrived(col_copy, slot, in_span)
        sent(col_copy, slot, in_span)
        marks = [empty] * col_packs
        halos = [merged(s.col_in[slot, 0, p], s.col_in[slot, 1, p]) for p in range(col_packs)]
        for z in range(2, layers):
            c = s.field[slot, z]
            beside = around(c, s.row_in[slot, 0, z:z + 1, :], s.row_in[slot, 1, z:z + 1, :],
                            unpacked(halos, col_place(z)))
            beside = beside + s.field[slot, z - 1] + s.field[slot, z + 1]
            new = c + KAPPA * (beside - 6.0 * c) + gen_ref[z]
            s.field[later, z] = new
            note_rows(z, new)
            marks = packed(marks, new, col_place(z))
        for p in range(col_packs):
            s.col_out[p] = marks[p]

        @pl.when(more)
        def _():
            start(row_copy, later, in_flow)
            start(col_copy, later, in_span)

        @pl.when(turn > 0)
        def _():
            for hop in range(2, flow - 1):
                layer_copy(held, hop).wait_recv()
        arrived(side_copy, slot, in_span)
        sent(side_copy, slot, in_span)
        halos = [merged(s.side_in[slot, 0, p], s.side_in[slot, 1, p]) for p in range(packs)]
        side_marks = [empty] * packs
        for b in range(flow):
            c = s.plane[slot, b]
            low = s.plane[slot, b - 1, block - 1:block, :] if b else jnp.zeros((1, seg), F32)
            high = s.plane[slot, b + 1, 0:1, :] if b < flow - 1 else jnp.zeros((1, seg), F32)
            beside = around(c, low, high, unpacked(halos, side_place(b))) + s.one[held, b]
            new = c + KAPPA * (beside - 6.0 * c) + s.gen0[b] - sinks(b)
            s.plane[later, b] = new
            side_marks = packed(side_marks, new, side_place(b))
            hi, lo = split(new)
            s.base[b * block:(b + 1) * block, 0:seg] = hi
            s.base[b * block:(b + 1) * block, seg:2 * seg] = lo
        for p in range(packs):
            s.side_out[p] = side_marks[p]

        @pl.when(more)
        def _():
            start(side_copy, later, in_span)
        return carry

    lax.fori_loop(0, STEPS, step, 0)
    for kind in range(len(kinds)):
        for hop in range(1, half):
            direct(kind, hop).wait_send()
            if kind != 2:
                relay(kind, hop).wait_send()
        to_mate(kind).wait_send()
    last = STEPS % 2
    solid_out[0] = s.plane[last, me]
    for z in range(1, layers):
        solid_out[z] = s.field[last, z]
    rows = pl.ds(pl.multiple_of(me * channels, channels), channels)
    for t in range(count):
        cols = slice(t * seg, (t + 1) * seg)
        first = s.run[t, rows, :] + s.reach[me, :, cols] * s.enter[me]
        cool_out[:, cols] = s.fall[me, :, cols] * (s.part[t, rows, :] + s.fore[me, :, cols] * first)


class Scratch:
    pass


def body(solid_start, heat_gen, conductance, heat_capacity, inlet_temp, wall_owner, wall_row):
    flow = lax.axis_size("flow")
    span = lax.axis_size("span")
    layers, block, seg = solid_start.shape
    channels, stations = conductance.shape
    count = stations // seg
    segs = channels * count
    width = flow * channels
    total = count * width
    cells = flow * block
    half = flow // 2
    lines = cells // 8
    keep = cells * total * 4 <= (8 << 20)
    group = max(1, 512 // width)
    packs = -(-lines // (seg // 2))
    col_packs = -(-(block // 8) // (seg // 2 // layers))
    dims = (flow, span, layers, block, seg, channels, count, group, keep)
    vm = pltpu.VMEM
    dma = pltpu.SemaphoreType.DMA
    march = vm((flow, channels, stations), F32)
    parts = vm((count, width, seg), F32)
    scratch = dict(
        idx_own=vm((8, seg), F32), idx=vm((flow, 8, seg), F32), first=vm((flow, 2, block, seg), F32),
        gen0=vm((flow, block, seg), F32), one=vm((4, flow, block, seg), F32),
        plane=vm((2, flow, block, seg), F32), field=vm((2, layers + 1, block, seg), F32),
        side_out=vm((packs, 8, seg), F32), side_in=vm((2, 2, packs, 8, seg), F32),
        rim_out=vm((8, seg), F32), rim_in=vm((2, 2, 8, seg), F32),
        col_out=vm((col_packs, 8, seg), F32), col_in=vm((2, 2, col_packs, 8, seg), F32),
        row_out=vm((2, layers, seg), F32), row_in=vm((2, 2, layers, seg), F32),
        tri=vm((2 * seg, 2 * seg), BF16), seats=vm((flow, channels, 2 * seg), BF16),
        along=vm((count, width), F32),
        take=vm((total, cells), BF16) if keep else parts,
        base=vm((cells, 2 * seg), BF16), heat=vm((total, 2 * seg), BF16),
        gain=march, fall=march, heat_of=march, fore=march, rear=march, reach=march,
        whole=vm((flow, channels, seg), F32), enter=vm((flow, channels, seg), F32),
        wall=parts, part=parts, run=parts,
        once_send=dma((4, flow - 1)), once_recv=dma((4, flow - 1)),
        one_send=dma((flow - 1,)), one_recv=dma((4, flow - 1)),
        side_send=dma((2,)), side_recv=dma((2, 2)), rim_send=dma((2,)), rim_recv=dma((2, 2)),
        col_send=dma((2,)), col_recv=dma((2, 2)), row_send=dma((2,)), row_recv=dma((2, 2)),
    )
    if keep:
        scratch["give"] = vm((cells, total), BF16)
    names = list(scratch)

    def run(*refs):
        held = Scratch()
        for name, ref in zip(names, refs[9:]):
            setattr(held, name, ref)
        kernel(dims, *refs[:9], held)

    return pl.pallas_call(
        run,
        out_shape=(jax.ShapeDtypeStruct(solid_start.shape, F32),
                   jax.ShapeDtypeStruct(conductance.shape, F32)),
        in_specs=[pl.BlockSpec(memory_space=pltpu.VMEM)] * 7,
        out_specs=(pl.BlockSpec(memory_space=pltpu.VMEM),) * 2,
        scratch_shapes=list(scratch.values()),
        compiler_params=pltpu.CompilerParams(
            collective_id=0, has_side_effects=True, vmem_limit_bytes=63 << 20),
    )(wall_owner.reshape(segs // seg, seg), wall_row.reshape(segs // seg, seg),
      heat_capacity.reshape(1, channels), inlet_temp.reshape(1, channels),
      conductance, solid_start, heat_gen)


def solution(mesh):
    placed = (
        P(None, "flow", "span"),
        P(None, "flow", "span"),
        P("span", "flow"),
        P("span"),
        P("span"),
        P(("flow", "span"), None),
        P(("flow", "span"), None),
    )
    return jax.shard_map(
        body,
        mesh=mesh,
        in_specs=placed,
        out_specs=(P(None, "flow", "span"), P("span", "flow")),
        check_vma=False,
    )
```

```python
import jax
import jax.numpy as jnp
from jax import lax
from jax.experimental import pallas as pl
from jax.experimental.pallas import tpu as pltpu
from jax.sharding import PartitionSpec as P

STEPS = 10
PARTS = 4
KAPPA = 0.16
MESH = pl.DeviceIdType.MESH
F32 = jnp.float32
BF16 = jnp.bfloat16


def split(x):
    hi = x.astype(BF16)
    lo = (x - hi.astype(F32)).astype(BF16)
    return hi, lo


def kernel(dims, owner_ref, row_ref, cap_ref, inlet_ref, cond_ref, start_ref, gen_ref,
           solid_out, cool_out, s):
    flow, span, layers, block, seg, channels, count, group, keep = dims
    width = flow * channels
    cells = flow * block
    half = flow // 2
    tiles = block // 8
    lines = cells // 8
    packs = -(-lines // (seg // 2))
    deep = layers // PARTS
    me = lax.axis_index("flow")
    at = lax.axis_index("span")
    mate = me + 1 - 2 * lax.rem(me, 2)
    above, below = at > 0, at < span - 1
    before, after = me > 0, me < flow - 1

    lane = lax.broadcasted_iota(jnp.int32, (8, seg), 1)
    pair = lane // 2
    lane_b = lax.broadcasted_iota(jnp.int32, (block, seg), 1)
    row_b = lax.broadcasted_iota(jnp.int32, (block, seg), 0)
    first_b, last_b = lane_b == 0, lane_b == seg - 1
    top_b, low_b = row_b == 0, row_b == block - 1

    def remote(src, dst, send, recv, device):
        return pltpu.make_async_remote_copy(
            src_ref=src, dst_ref=dst, send_sem=send, recv_sem=recv,
            device_id=device, device_id_type=MESH)

    kinds = (
        (s.idx_own, lambda f: s.idx.at[f]),
        (start_ref.at[0], lambda f: s.plane.at[0, f]),
        (cond_ref, lambda f: s.gain.at[f]),
        (start_ref.at[1], lambda f: s.one.at[0, f]),
        (gen_ref.at[0], lambda f: s.gen0.at[f]),
    )

    def direct(kind, hop):
        src, dst = kinds[kind]
        to = lax.rem(me + 2 * hop, flow)
        return remote(src, dst(me), s.once_send.at[kind, 2 * hop - 1], s.once_recv.at[kind, 2 * hop - 1], (to, at))

    def to_mate(kind):
        src, dst = kinds[kind]
        return remote(src, dst(me), s.once_send.at[kind, 0], s.once_recv.at[kind, 0], (mate, at))

    def relay(kind, hop):
        _, dst = kinds[kind]
        origin = lax.rem(me + flow - 2 * hop, flow)
        return remote(dst(origin), dst(origin), s.once_send.at[kind, 2 * hop], s.once_recv.at[kind, 2 * hop], (mate, at))

    def one_direct(slot, hop):
        to = lax.rem(me + 2 * hop, flow)
        return remote(s.one.at[slot, me], s.one.at[slot, me],
                      s.one_send.at[2 * hop - 1], s.one_recv.at[slot, 2 * hop - 1], (to, at))

    def one_to_mate(slot):
        return remote(s.one.at[slot, me], s.one.at[slot, me],
                      s.one_send.at[0], s.one_recv.at[slot, 0], (mate, at))

    def one_relay(slot, hop):
        origin = lax.rem(me + flow - 2 * hop, flow)
        return remote(s.one.at[slot, origin], s.one.at[slot, origin],
                      s.one_send.at[2 * hop], s.one_recv.at[slot, 2 * hop], (mate, at))

    def side_copy(slot, side):
        return remote(s.side_out, s.side_in.at[slot, 1 - side],
                      s.side_send.at[side], s.side_recv.at[slot, 1 - side], (me, at - 1 + 2 * side))

    def col_copy(part):
        def copy(slot, side):
            return remote(s.col_out.at[part], s.col_in.at[slot, part, 1 - side],
                          s.col_send.at[part, side], s.col_recv.at[slot, part, 1 - side], (me, at - 1 + 2 * side))
        return copy

    def row_copy(part):
        rows = pl.ds(part * deep, deep)

        def copy(slot, side):
            return remote(s.row_out.at[side, rows], s.row_in.at[slot, 1 - side, rows],
                          s.row_send.at[part, side], s.row_recv.at[slot, part, 1 - side], (me - 1 + 2 * side, at))
        return copy

    def both(copy, pair_of, act):
        for side, there in enumerate(pair_of):
            @pl.when(there)
            def _():
                act(copy, side)

    in_span, in_flow = (above, below), (before, after)

    def start(copy, slot, pair_of):
        both(copy, pair_of, lambda c, side: c(slot, side).start())

    def sent(copy, slot, pair_of):
        both(copy, pair_of, lambda c, side: c(slot, side).wait_send())

    def arrived(copy, slot, pair_of):
        both(copy, pair_of, lambda c, side: c(slot, 1 - side).wait_recv())

    s.side_in[...] = jnp.zeros_like(s.side_in)
    s.col_in[...] = jnp.zeros_like(s.col_in)
    s.row_in[...] = jnp.zeros_like(s.row_in)
    s.idx_own[...] = jnp.zeros_like(s.idx_own)
    per = owner_ref.shape[0]
    s.idx_own[0:per, :] = owner_ref[...].astype(F32)
    s.idx_own[per:2 * per, :] = row_ref[...].astype(F32)
    barrier = pltpu.get_barrier_semaphore()
    for hop in range(1, flow):
        pl.semaphore_signal(barrier, inc=1, device_id=(lax.rem(me + hop, flow), at), device_id_type=MESH)
    for side, there in enumerate(in_span):
        @pl.when(there)
        def _():
            pl.semaphore_signal(barrier, inc=1, device_id=(me, at - 1 + 2 * side), device_id_type=MESH)
    pl.semaphore_wait(barrier, flow - 1 + above.astype(jnp.int32) + below.astype(jnp.int32))
    for kind in range(len(kinds)):
        for hop in range(1, half):
            direct(kind, hop).start()
        to_mate(kind).start()
    s.idx[me] = s.idx_own[...]
    s.plane[0, me] = start_ref[0]
    s.one[0, me] = start_ref[1]
    s.gain[me] = cond_ref[...]
    s.gen0[me] = gen_ref[0]

    def packed(marks, value, place):
        for r in range(tiles):
            p, k = place(r)
            turned = pltpu.roll(value[8 * r:8 * r + 8], 2 * k + 1, 1)
            marks[p] = jnp.where(pair == k, turned, marks[p])
        return marks

    def merged(low, high):
        return jnp.where(lax.rem(lane, 2) == 0, pltpu.roll(high, seg - 1, 1), pltpu.roll(low, 1, 1))

    def unpacked(marks, place):
        return jnp.concatenate(
            [pltpu.roll(marks[p], seg - 1 - 2 * k, 1) for p, k in (place(r) for r in range(tiles))], axis=0)

    def col_place(z):
        per_pack = seg // 2 // deep
        return lambda r: (r // per_pack, z % deep + deep * (r % per_pack))

    def side_place(b):
        return lambda r: divmod(b * tiles + r, seg // 2)

    col_packs = s.col_out.shape[1]
    empty = jnp.zeros((8, seg), F32)

    def around(c, low_row, high_row, halo):
        beside = jnp.where(top_b, low_row, pltpu.roll(c, 1, 0))
        beside = beside + jnp.where(low_b, high_row, pltpu.roll(c, block - 1, 0))
        beside = beside + jnp.where(first_b, halo, pltpu.roll(c, 1, 1))
        return beside + jnp.where(last_b, halo, pltpu.roll(c, seg - 1, 1))

    for side in range(2):
        s.row_out[side] = jnp.zeros_like(s.row_out[side])
    s.field[0, layers] = jnp.zeros((block, seg), F32)
    s.field[1, layers] = jnp.zeros((block, seg), F32)

    def note_rows(z, new):
        s.row_out[0, z:z + 1, :] = new[0:1, :]
        s.row_out[1, z:z + 1, :] = new[block - 1:block, :]

    def members(part):
        return range(max(1, part * deep), (part + 1) * deep)

    def send_part(part, slot):
        start(row_copy(part), slot, in_flow)
        start(col_copy(part), slot, in_span)

    for part in range(PARTS):
        marks = [empty] * col_packs
        for z in members(part):
            new = start_ref[z]
            s.field[0, z] = new
            note_rows(z, new)
            marks = packed(marks, new, col_place(z))
        for p in range(col_packs):
            s.col_out[part, p] = marks[p]
        send_part(part, 0)

    mid = seg // 2 - 1
    i2 = lax.rem(lax.broadcasted_iota(jnp.int32, (2 * seg, 2 * seg), 0), seg)
    j2 = lax.broadcasted_iota(jnp.int32, (2 * seg, 2 * seg), 1)
    tri = jnp.where((i2 <= j2) | (j2 >= seg), 1.0, 0.0).astype(BF16)
    s.tri[...] = tri
    i3 = lax.rem(lax.broadcasted_iota(jnp.int32, (3 * seg, 3 * seg), 0), seg)
    j3 = lax.broadcasted_iota(jnp.int32, (3 * seg, 3 * seg), 1)
    lower = jnp.where(i3 <= mid, 1.0, 0.0)
    spread = jnp.where(j3 < seg, jnp.where(i3 <= j3, 1.0, 0.0) - lower,
                       jnp.where(j3 < 2 * seg, lower, 1.0 - lower)).astype(BF16)
    eye = (lax.broadcasted_iota(jnp.int32, (channels, channels), 0)
           == lax.broadcasted_iota(jnp.int32, (channels, channels), 1))

    def column(ref):
        wide = jnp.where(eye, jnp.broadcast_to(ref[...], (channels, channels)), 0.0)
        return jnp.broadcast_to(jnp.sum(wide, axis=1, keepdims=True), (channels, seg))

    capacity, inlet = column(cap_ref), column(inlet_ref)

    def hand_on(kind, hop):
        direct(kind, hop).wait_recv()
        relay(kind, hop).start()

    def pass_on(kind):
        for hop in range(1, half):
            hand_on(kind, hop)

    def take_in(kind):
        to_mate(kind).wait_recv()
        for hop in range(1, half):
            relay(kind, hop).wait_recv()

    pass_on(0)
    pass_on(1)
    take_in(0)
    share = seg // count
    lane_i = lax.broadcasted_iota(jnp.int32, (channels, seg), 1) // count
    chan_i = lax.rem(lax.broadcasted_iota(jnp.int32, (channels, seg), 0), share)
    here = lane_i == chan_i

    def one_source(f, carry):
        def taken(base):
            rows = jnp.concatenate(
                [jnp.broadcast_to(s.idx[f, base + a:base + a + 1, :], (share, seg)) for a in range(per)], axis=0)
            return jnp.where(here, rows, 0.0).astype(BF16)
        s.seats[f] = jnp.concatenate([taken(0), taken(per)], axis=1)
        return carry

    lax.fori_loop(0, flow, one_source, 0)
    seats = s.seats[...].reshape(width, 2 * seg)
    ci = lax.broadcasted_iota(jnp.int32, (2 * seg, seg), 0)
    weight = jnp.where(ci < seg, float(block), 1.0)
    turn_of = lax.rem(ci, count)
    ri = lax.broadcasted_iota(jnp.int32, (count, 2 * seg), 1)
    rt = lax.broadcasted_iota(jnp.int32, (count, 2 * seg), 0)
    pick = jnp.where(lax.rem(ri, count) == rt, jnp.where(ri < seg, float(block), 1.0), 0.0).astype(BF16)
    s.along[...] = lax.dot_general(pick, seats, (((1,), (1,)), ((), ())), preferred_element_type=F32)

    def one_turn(t, carry):
        chosen = jnp.where(turn_of == t, weight, 0.0).astype(BF16)
        cell = jnp.dot(seats, chosen, preferred_element_type=F32)
        if keep:
            lanes = lax.broadcasted_iota(jnp.int32, (width, seg), 1).astype(F32)
            rows = pl.ds(pl.multiple_of(t * width, width), width)
            for k in range(cells // seg):
                s.take[rows, k * seg:(k + 1) * seg] = jnp.where(cell - float(k * seg) == lanes, 1.0, 0.0).astype(BF16)
        else:
            s.take[t] = cell
        return carry

    lax.fori_loop(0, count, one_turn, 0)
    if keep:
        for t in range(count):
            for b in range(flow):
                rows = lax.broadcasted_iota(jnp.int32, (block, width), 0).astype(F32) + float(b * block)
                s.give[b * block:(b + 1) * block, t * width:(t + 1) * width] = jnp.where(
                    rows == s.along[t:t + 1, :], 1.0, 0.0).astype(BF16)

    def take_rows(t0):
        if keep:
            return s.take[t0 * width:(t0 + group) * width, :]
        cell = s.take[t0:t0 + group].reshape(group * width, seg)
        lanes = lax.broadcasted_iota(jnp.int32, (group * width, seg), 1).astype(F32)
        return jnp.concatenate(
            [jnp.where(cell - float(k * seg) == lanes, 1.0, 0.0).astype(BF16) for k in range(cells // seg)], axis=1)

    def give_rows(t0, b):
        if keep:
            return s.give[b * block:(b + 1) * block, t0 * width:(t0 + group) * width]
        rows = lax.broadcasted_iota(jnp.int32, (block, width), 0).astype(F32) + float(b * block)
        return jnp.concatenate(
            [jnp.where(rows == s.along[t:t + 1, :], 1.0, 0.0).astype(BF16) for t in range(t0, t0 + group)], axis=1)

    take_in(1)

    side_marks = [empty] * packs
    for b in range(flow):
        c = s.plane[0, b]
        side_marks = packed(side_marks, c, side_place(b))
        hi, lo = split(c)
        s.base[b * block:(b + 1) * block, 0:seg] = hi
        s.base[b * block:(b + 1) * block, seg:2 * seg] = lo
    for p in range(packs):
        s.side_out[p] = side_marks[p]
    start(side_copy, 0, in_span)

    def chunk(ref, t):
        return ref[:, :, t * seg:(t + 1) * seg].reshape(width, seg)

    def constants(i, carry):
        own_core = jnp.logical_and(i >= 2, i <= half)
        hop = jnp.where(i < 2, 0, jnp.where(i <= half, i - 1, i - half))
        from_me = lax.rem(me + flow - 2 * hop, flow)
        from_mate = lax.rem(mate + flow - 2 * hop, flow)
        f = jnp.where(jnp.logical_or(i == 0, own_core), from_me, from_mate)

        @pl.when(i == 1)
        def _():
            to_mate(2).wait_recv()

        @pl.when(own_core)
        def _():
            hand_on(2, hop)

        @pl.when(i > half)
        def _():
            relay(2, hop).wait_recv()

        @pl.when(own_core)
        def _():
            relay(2, hop).wait_send()

        k = jnp.concatenate([s.gain[f, :, t * seg:(t + 1) * seg] for t in range(count)], axis=0)
        k1 = k.astype(BF16)
        rest = k - k1.astype(F32)
        k2 = rest.astype(BF16)
        k3 = (rest - k2.astype(F32)).astype(BF16)
        sums = jnp.dot(jnp.concatenate([k1, k2, k3], axis=1), spread, preferred_element_type=F32)
        run = jnp.ones((channels, seg), F32)
        for t in range(count):
            rows = slice(t * channels, (t + 1) * channels)
            cols = slice(t * seg, (t + 1) * seg)
            kt, depth = k[rows], sums[rows, 0:seg]
            fore, rear = jnp.exp(-sums[rows, seg:2 * seg]), jnp.exp(-sums[rows, 2 * seg:])
            s.gain[f, :, cols] = (1.0 - jnp.exp(-kt)) * jnp.exp(depth)
            s.fall[f, :, cols] = jnp.exp(-depth)
            s.heat_of[f, :, cols] = (jnp.exp(kt) - 1.0) * capacity
            s.fore[f, :, cols] = fore
            s.rear[f, :, cols] = rear
            s.reach[f, :, cols] = run
            run = run * (fore * rear)
        s.whole[f] = run
        return carry

    lax.fori_loop(0, flow, constants, 0)

    def march(run, first_t, last_t):
        base = s.base[...]
        for t0 in range(first_t, last_t, group):
            found = jnp.dot(take_rows(t0), base, preferred_element_type=F32)
            w = found[:, :seg] + found[:, seg:]
            gains = jnp.concatenate([chunk(s.gain, t) for t in range(t0, t0 + group)], axis=0)
            hi, lo = split(gains * w)
            sums = jnp.dot(jnp.concatenate([hi, lo], axis=1), s.tri[...], preferred_element_type=F32)
            for i in range(group):
                t = t0 + i
                rows = slice(i * width, (i + 1) * width)
                s.wall[t] = w[rows]
                s.part[t] = sums[rows, :seg]
                s.run[t] = run
                run = chunk(s.rear, t) * (sums[rows, seg:] + chunk(s.fore, t) * run)
        return run

    def heats(run):
        enter = inlet
        for f in range(flow):
            s.enter[f] = enter
            enter = run[f * channels:(f + 1) * channels] + s.whole[f] * enter
        enter = s.enter[...].reshape(width, seg)
        for t0 in range(0, count, group):
            for t in range(t0, t0 + group):
                first = s.run[t] + chunk(s.reach, t) * enter
                cool = chunk(s.fall, t) * (s.part[t] + chunk(s.fore, t) * first)
                hi, lo = split(chunk(s.heat_of, t) * (s.wall[t] - cool))
                s.heat[t * width:(t + 1) * width, 0:seg] = hi
                s.heat[t * width:(t + 1) * width, seg:2 * seg] = lo

    def sinks():
        if keep:
            total = jnp.dot(s.give[...], s.heat[...], preferred_element_type=F32)
            s.sink[...] = total[:, :seg] + total[:, seg:]
            return
        for b in range(flow):
            total = jnp.zeros((block, 2 * seg), F32)
            for t0 in range(0, count, group):
                total = total + jnp.dot(give_rows(t0, b), s.heat[t0 * width:(t0 + group) * width, :],
                                        preferred_element_type=F32)
            s.sink[b * block:(b + 1) * block, :] = total[:, :seg] + total[:, seg:]

    def await_part(part, slot):
        arrived(row_copy(part), slot, in_flow)
        sent(row_copy(part), slot, in_flow)
        arrived(col_copy(part), slot, in_span)
        sent(col_copy(part), slot, in_span)

    def conduct(part, slot, later):
        marks = [empty] * col_packs
        halos = [merged(s.col_in[slot, part, 0, p], s.col_in[slot, part, 1, p]) for p in range(col_packs)]
        for z in members(part):
            c = s.field[slot, z]
            beside = around(c, s.row_in[slot, 0, z:z + 1, :], s.row_in[slot, 1, z:z + 1, :],
                            unpacked(halos, col_place(z)))
            under = s.plane[slot, me] if z == 1 else s.field[slot, z - 1]
            beside = beside + under + s.field[slot, z + 1]
            new = c + KAPPA * (beside - 6.0 * c) + gen_ref[z]
            s.field[later, z] = new
            note_rows(z, new)
            marks = packed(marks, new, col_place(z))
        for p in range(col_packs):
            s.col_out[part, p] = marks[p]

    def step(turn, carry):
        slot, later = lax.rem(turn, 2), lax.rem(turn + 1, 2)
        held, next_held = lax.rem(turn, 4), lax.rem(turn + 1, 4)
        more = turn < STEPS - 1

        await_part(0, slot)
        run = march(jnp.zeros((width, seg), F32), 0, count // 2)
        conduct(0, slot, later)

        @pl.when(turn > 0)
        def _():
            for hop in range(1, half):
                one_direct(held, hop).wait_send()
            one_to_mate(held).wait_send()

        @pl.when(turn > 1)
        def _():
            for hop in range(1, half):
                one_relay(held, hop).wait_send()
        s.one[next_held, me] = s.field[later, 1]

        @pl.when(more)
        def _():
            send_part(0, later)
            for hop in range(1, half):
                one_direct(next_held, hop).start()
            one_to_mate(next_held).start()
        await_part(1, slot)
        run = march(run, count // 2, count)
        conduct(1, slot, later)

        @pl.when(turn > 0)
        def _():
            for hop in range(1, half):
                one_direct(held, hop).wait_recv()
                one_relay(held, hop).start()

        @pl.when(turn == 0)
        def _():
            pass_on(3)
            pass_on(4)

        @pl.when(more)
        def _():
            send_part(1, later)
        await_part(2, slot)
        heats(run)
        conduct(2, slot, later)

        @pl.when(more)
        def _():
            send_part(2, later)
        await_part(3, slot)
        sinks()
        conduct(3, slot, later)

        @pl.when(more)
        def _():
            send_part(3, later)

        @pl.when(turn == 0)
        def _():
            take_in(3)
            take_in(4)
            for hop in range(1, half):
                relay(1, hop).wait_send()
                relay(3, hop).wait_send()

        @pl.when(turn > 0)
        def _():
            one_to_mate(held).wait_recv()
            for hop in range(1, half):
                one_relay(held, hop).wait_recv()
        arrived(side_copy, slot, in_span)
        sent(side_copy, slot, in_span)
        halos = [merged(s.side_in[slot, 0, p], s.side_in[slot, 1, p]) for p in range(packs)]
        side_marks = [empty] * packs
        for b in range(flow):
            c = s.plane[slot, b]
            low = s.plane[slot, b - 1, block - 1:block, :] if b else jnp.zeros((1, seg), F32)
            high = s.plane[slot, b + 1, 0:1, :] if b < flow - 1 else jnp.zeros((1, seg), F32)
            beside = around(c, low, high, unpacked(halos, side_place(b))) + s.one[held, b]
            new = c + KAPPA * (beside - 6.0 * c) + s.gen0[b] - s.sink[b * block:(b + 1) * block, :]
            s.plane[later, b] = new
            side_marks = packed(side_marks, new, side_place(b))
            hi, lo = split(new)
            s.base[b * block:(b + 1) * block, 0:seg] = hi
            s.base[b * block:(b + 1) * block, seg:2 * seg] = lo
        for p in range(packs):
            s.side_out[p] = side_marks[p]

        @pl.when(more)
        def _():
            start(side_copy, later, in_span)
        return carry

    lax.fori_loop(0, STEPS, step, 0)
    for kind in range(len(kinds)):
        for hop in range(1, half):
            direct(kind, hop).wait_send()
            if kind in (0, 4):
                relay(kind, hop).wait_send()
        to_mate(kind).wait_send()
    for hop in range(1, half):
        one_relay(0, hop).wait_send()
    last = STEPS % 2
    solid_out[0] = s.plane[last, me]
    for z in range(1, layers):
        solid_out[z] = s.field[last, z]
    rows = pl.ds(pl.multiple_of(me * channels, channels), channels)
    for t in range(count):
        cols = slice(t * seg, (t + 1) * seg)
        first = s.run[t, rows, :] + s.reach[me, :, cols] * s.enter[me]
        cool_out[:, cols] = s.fall[me, :, cols] * (s.part[t, rows, :] + s.fore[me, :, cols] * first)


class Scratch:
    pass


def body(solid_start, heat_gen, conductance, heat_capacity, inlet_temp, wall_owner, wall_row):
    flow = lax.axis_size("flow")
    span = lax.axis_size("span")
    layers, block, seg = solid_start.shape
    channels, stations = conductance.shape
    count = stations // seg
    segs = channels * count
    width = flow * channels
    total = count * width
    cells = flow * block
    half = flow // 2
    lines = cells // 8
    keep = cells * total * 4 <= (8 << 20)
    group = max(1, 512 // width)
    packs = -(-lines // (seg // 2))
    col_packs = -(-(block // 8) // (seg // 2 // (layers // PARTS)))
    dims = (flow, span, layers, block, seg, channels, count, group, keep)
    vm = pltpu.VMEM
    dma = pltpu.SemaphoreType.DMA
    march = vm((flow, channels, stations), F32)
    parts = vm((count, width, seg), F32)
    scratch = dict(
        idx_own=vm((8, seg), F32), idx=vm((flow, 8, seg), F32),
        gen0=vm((flow, block, seg), F32), one=vm((4, flow, block, seg), F32),
        plane=vm((2, flow, block, seg), F32), field=vm((2, layers + 1, block, seg), F32),
        side_out=vm((packs, 8, seg), F32), side_in=vm((2, 2, packs, 8, seg), F32),
        sink=vm((cells, seg), F32),
        col_out=vm((PARTS, col_packs, 8, seg), F32), col_in=vm((2, PARTS, 2, col_packs, 8, seg), F32),
        row_out=vm((2, layers, seg), F32), row_in=vm((2, 2, layers, seg), F32),
        tri=vm((2 * seg, 2 * seg), BF16), seats=vm((flow, channels, 2 * seg), BF16),
        along=vm((count, width), F32),
        take=vm((total, cells), BF16) if keep else parts,
        base=vm((cells, 2 * seg), BF16), heat=vm((total, 2 * seg), BF16),
        gain=march, fall=march, heat_of=march, fore=march, rear=march, reach=march,
        whole=vm((flow, channels, seg), F32), enter=vm((flow, channels, seg), F32),
        wall=parts, part=parts, run=parts,
        once_send=dma((5, flow - 1)), once_recv=dma((5, flow - 1)),
        one_send=dma((flow - 1,)), one_recv=dma((4, flow - 1)),
        side_send=dma((2,)), side_recv=dma((2, 2)),
        col_send=dma((PARTS, 2)), col_recv=dma((2, PARTS, 2)),
        row_send=dma((PARTS, 2)), row_recv=dma((2, PARTS, 2)),
    )
    if keep:
        scratch["give"] = vm((cells, total), BF16)
    names = list(scratch)

    def run(*refs):
        held = Scratch()
        for name, ref in zip(names, refs[9:]):
            setattr(held, name, ref)
        kernel(dims, *refs[:9], held)

    return pl.pallas_call(
        run,
        out_shape=(jax.ShapeDtypeStruct(solid_start.shape, F32),
                   jax.ShapeDtypeStruct(conductance.shape, F32)),
        in_specs=[pl.BlockSpec(memory_space=pltpu.VMEM)] * 7,
        out_specs=(pl.BlockSpec(memory_space=pltpu.VMEM),) * 2,
        scratch_shapes=list(scratch.values()),
        compiler_params=pltpu.CompilerParams(
            collective_id=0, has_side_effects=True, vmem_limit_bytes=63 << 20),
    )(wall_owner.reshape(segs // seg, seg), wall_row.reshape(segs // seg, seg),
      heat_capacity.reshape(1, channels), inlet_temp.reshape(1, channels),
      conductance, solid_start, heat_gen)


def solution(mesh):
    placed = (
        P(None, "flow", "span"),
        P(None, "flow", "span"),
        P("span", "flow"),
        P("span"),
        P("span"),
        P(("flow", "span"), None),
        P(("flow", "span"), None),
    )
    return jax.shard_map(
        body,
        mesh=mesh,
        in_specs=placed,
        out_specs=(P(None, "flow", "span"), P("span", "flow")),
        check_vma=False,
    )
```

```python
import jax
import jax.numpy as jnp
from jax import lax
from jax.experimental import pallas as pl
from jax.experimental.pallas import tpu as pltpu
from jax.sharding import PartitionSpec as P

STEPS = 10
PARTS = 4
KAPPA = 0.16
MESH = pl.DeviceIdType.MESH
F32 = jnp.float32
BF16 = jnp.bfloat16


def split(x):
    hi = x.astype(BF16)
    lo = (x - hi.astype(F32)).astype(BF16)
    return hi, lo


def kernel(dims, owner_ref, row_ref, cap_ref, inlet_ref, cond_ref, start_ref, gen_ref,
           solid_out, cool_out, s):
    flow, span, layers, block, seg, channels, count, group, keep = dims
    width = flow * channels
    cells = flow * block
    half = flow // 2
    tiles = block // 8
    lines = cells // 8
    packs = -(-lines // (seg // 2))
    deep = layers // PARTS
    me = lax.axis_index("flow")
    at = lax.axis_index("span")
    mate = me + 1 - 2 * lax.rem(me, 2)
    above, below = at > 0, at < span - 1
    before, after = me > 0, me < flow - 1

    lane = lax.broadcasted_iota(jnp.int32, (8, seg), 1)
    pair = lane // 2
    lane_b = lax.broadcasted_iota(jnp.int32, (block, seg), 1)
    row_b = lax.broadcasted_iota(jnp.int32, (block, seg), 0)
    first_b, last_b = lane_b == 0, lane_b == seg - 1
    top_b, low_b = row_b == 0, row_b == block - 1

    def remote(src, dst, send, recv, device):
        return pltpu.make_async_remote_copy(
            src_ref=src, dst_ref=dst, send_sem=send, recv_sem=recv,
            device_id=device, device_id_type=MESH)

    kinds = (
        (s.idx_own, lambda f: s.idx.at[f]),
        (start_ref.at[0], lambda f: s.plane.at[0, f]),
        (cond_ref, lambda f: s.gain.at[f]),
        (start_ref.at[1], lambda f: s.one.at[0, f]),
        (gen_ref.at[0], lambda f: s.gen0.at[f]),
    )

    def direct(kind, hop):
        src, dst = kinds[kind]
        to = lax.rem(me + 2 * hop, flow)
        return remote(src, dst(me), s.once_send.at[kind, 2 * hop - 1], s.once_recv.at[kind, 2 * hop - 1], (to, at))

    def to_mate(kind):
        src, dst = kinds[kind]
        return remote(src, dst(me), s.once_send.at[kind, 0], s.once_recv.at[kind, 0], (mate, at))

    def relay(kind, hop):
        _, dst = kinds[kind]
        origin = lax.rem(me + flow - 2 * hop, flow)
        return remote(dst(origin), dst(origin), s.once_send.at[kind, 2 * hop], s.once_recv.at[kind, 2 * hop], (mate, at))

    def one_direct(slot, hop):
        to = lax.rem(me + 2 * hop, flow)
        return remote(s.one.at[slot, me], s.one.at[slot, me],
                      s.one_send.at[2 * hop - 1], s.one_recv.at[slot, 2 * hop - 1], (to, at))

    def one_to_mate(slot):
        return remote(s.one.at[slot, me], s.one.at[slot, me],
                      s.one_send.at[0], s.one_recv.at[slot, 0], (mate, at))

    def one_relay(slot, hop):
        origin = lax.rem(me + flow - 2 * hop, flow)
        return remote(s.one.at[slot, origin], s.one.at[slot, origin],
                      s.one_send.at[2 * hop], s.one_recv.at[slot, 2 * hop], (mate, at))

    def side_copy(slot, side):
        return remote(s.side_out, s.side_in.at[slot, 1 - side],
                      s.side_send.at[side], s.side_recv.at[slot, 1 - side], (me, at - 1 + 2 * side))

    def col_copy(part):
        def copy(slot, side):
            return remote(s.col_out.at[part], s.col_in.at[slot, part, 1 - side],
                          s.col_send.at[part, side], s.col_recv.at[slot, part, 1 - side], (me, at - 1 + 2 * side))
        return copy

    def row_copy(part):
        rows = pl.ds(part * deep, deep)

        def copy(slot, side):
            return remote(s.row_out.at[side, rows], s.row_in.at[slot, 1 - side, rows],
                          s.row_send.at[part, side], s.row_recv.at[slot, part, 1 - side], (me - 1 + 2 * side, at))
        return copy

    def both(copy, pair_of, act):
        for side, there in enumerate(pair_of):
            @pl.when(there)
            def _():
                act(copy, side)

    in_span, in_flow = (above, below), (before, after)

    def start(copy, slot, pair_of):
        both(copy, pair_of, lambda c, side: c(slot, side).start())

    def sent(copy, slot, pair_of):
        both(copy, pair_of, lambda c, side: c(slot, side).wait_send())

    def arrived(copy, slot, pair_of):
        both(copy, pair_of, lambda c, side: c(slot, 1 - side).wait_recv())

    s.side_in[...] = jnp.zeros_like(s.side_in)
    s.col_in[...] = jnp.zeros_like(s.col_in)
    s.row_in[...] = jnp.zeros_like(s.row_in)
    s.idx_own[...] = jnp.zeros_like(s.idx_own)
    per = owner_ref.shape[0]
    s.idx_own[0:per, :] = owner_ref[...].astype(F32)
    s.idx_own[per:2 * per, :] = row_ref[...].astype(F32)
    barrier = pltpu.get_barrier_semaphore()
    for hop in range(1, flow):
        pl.semaphore_signal(barrier, inc=1, device_id=(lax.rem(me + hop, flow), at), device_id_type=MESH)
    for side, there in enumerate(in_span):
        @pl.when(there)
        def _():
            pl.semaphore_signal(barrier, inc=1, device_id=(me, at - 1 + 2 * side), device_id_type=MESH)
    pl.semaphore_wait(barrier, flow - 1 + above.astype(jnp.int32) + below.astype(jnp.int32))
    for kind in range(len(kinds)):
        for hop in range(1, half):
            direct(kind, hop).start()
        to_mate(kind).start()
    s.idx[me] = s.idx_own[...]
    s.plane[0, me] = start_ref[0]
    s.one[0, me] = start_ref[1]
    s.gain[me] = cond_ref[...]
    s.gen0[me] = gen_ref[0]

    def packed(marks, value, place):
        for r in range(tiles):
            p, k = place(r)
            turned = pltpu.roll(value[8 * r:8 * r + 8], 2 * k + 1, 1)
            marks[p] = jnp.where(pair == k, turned, marks[p])
        return marks

    def merged(low, high):
        return jnp.where(lax.rem(lane, 2) == 0, pltpu.roll(high, seg - 1, 1), pltpu.roll(low, 1, 1))

    def unpacked(marks, place):
        return jnp.concatenate(
            [pltpu.roll(marks[p], seg - 1 - 2 * k, 1) for p, k in (place(r) for r in range(tiles))], axis=0)

    def col_place(z):
        per_pack = seg // 2 // deep
        return lambda r: (r // per_pack, z % deep + deep * (r % per_pack))

    def side_place(b):
        return lambda r: divmod(b * tiles + r, seg // 2)

    col_packs = s.col_out.shape[1]
    empty = jnp.zeros((8, seg), F32)

    def around(c, low_row, high_row, halo):
        beside = jnp.where(top_b, low_row, pltpu.roll(c, 1, 0))
        beside = beside + jnp.where(low_b, high_row, pltpu.roll(c, block - 1, 0))
        beside = beside + jnp.where(first_b, halo, pltpu.roll(c, 1, 1))
        return beside + jnp.where(last_b, halo, pltpu.roll(c, seg - 1, 1))

    for side in range(2):
        s.row_out[side] = jnp.zeros_like(s.row_out[side])
    s.field[0, layers] = jnp.zeros((block, seg), F32)
    s.field[1, layers] = jnp.zeros((block, seg), F32)

    def note_rows(z, new):
        s.row_out[0, z:z + 1, :] = new[0:1, :]
        s.row_out[1, z:z + 1, :] = new[block - 1:block, :]

    def members(part):
        return range(max(1, part * deep), (part + 1) * deep)

    def send_part(part, slot):
        start(row_copy(part), slot, in_flow)
        start(col_copy(part), slot, in_span)

    for part in range(PARTS):
        marks = [empty] * col_packs
        for z in members(part):
            new = start_ref[z]
            s.field[0, z] = new
            note_rows(z, new)
            marks = packed(marks, new, col_place(z))
        for p in range(col_packs):
            s.col_out[part, p] = marks[p]
        send_part(part, 0)

    mid = seg // 2 - 1
    i2 = lax.rem(lax.broadcasted_iota(jnp.int32, (2 * seg, 2 * seg), 0), seg)
    j2 = lax.broadcasted_iota(jnp.int32, (2 * seg, 2 * seg), 1)
    tri = jnp.where((i2 <= j2) | (j2 >= seg), 1.0, 0.0).astype(BF16)
    s.tri[...] = tri
    i3 = lax.rem(lax.broadcasted_iota(jnp.int32, (3 * seg, 3 * seg), 0), seg)
    j3 = lax.broadcasted_iota(jnp.int32, (3 * seg, 3 * seg), 1)
    lower = jnp.where(i3 <= mid, 1.0, 0.0)
    spread = jnp.where(j3 < seg, jnp.where(i3 <= j3, 1.0, 0.0) - lower,
                       jnp.where(j3 < 2 * seg, lower, 1.0 - lower)).astype(BF16)
    eye = (lax.broadcasted_iota(jnp.int32, (channels, channels), 0)
           == lax.broadcasted_iota(jnp.int32, (channels, channels), 1))

    def column(ref):
        wide = jnp.where(eye, jnp.broadcast_to(ref[...], (channels, channels)), 0.0)
        return jnp.broadcast_to(jnp.sum(wide, axis=1, keepdims=True), (channels, seg))

    capacity, inlet = column(cap_ref), column(inlet_ref)

    def hand_on(kind, hop):
        direct(kind, hop).wait_recv()
        relay(kind, hop).start()

    def pass_on(kind):
        for hop in range(1, half):
            hand_on(kind, hop)

    def take_in(kind):
        to_mate(kind).wait_recv()
        for hop in range(1, half):
            relay(kind, hop).wait_recv()

    pass_on(0)
    pass_on(1)
    take_in(0)
    share = seg // count
    lane_i = lax.broadcasted_iota(jnp.int32, (channels, seg), 1) // count
    chan_i = lax.rem(lax.broadcasted_iota(jnp.int32, (channels, seg), 0), share)
    here = lane_i == chan_i

    def one_source(f, carry):
        def taken(base):
            rows = jnp.concatenate(
                [jnp.broadcast_to(s.idx[f, base + a:base + a + 1, :], (share, seg)) for a in range(per)], axis=0)
            return jnp.where(here, rows, 0.0).astype(BF16)
        s.seats[f] = jnp.concatenate([taken(0), taken(per)], axis=1)
        return carry

    lax.fori_loop(0, flow, one_source, 0)
    seats = s.seats[...].reshape(width, 2 * seg)
    ci = lax.broadcasted_iota(jnp.int32, (2 * seg, seg), 0)
    weight = jnp.where(ci < seg, float(block), 1.0)
    turn_of = lax.rem(ci, count)
    ri = lax.broadcasted_iota(jnp.int32, (count, 2 * seg), 1)
    rt = lax.broadcasted_iota(jnp.int32, (count, 2 * seg), 0)
    pick = jnp.where(lax.rem(ri, count) == rt, jnp.where(ri < seg, float(block), 1.0), 0.0).astype(BF16)
    s.along[...] = lax.dot_general(pick, seats, (((1,), (1,)), ((), ())), preferred_element_type=F32)

    def one_turn(t, carry):
        chosen = jnp.where(turn_of == t, weight, 0.0).astype(BF16)
        cell = jnp.dot(seats, chosen, preferred_element_type=F32)
        if keep:
            lanes = lax.broadcasted_iota(jnp.int32, (width, seg), 1).astype(F32)
            rows = pl.ds(pl.multiple_of(t * width, width), width)
            for k in range(cells // seg):
                s.take[rows, k * seg:(k + 1) * seg] = jnp.where(cell - float(k * seg) == lanes, 1.0, 0.0).astype(BF16)
        else:
            s.take[t] = cell
        return carry

    lax.fori_loop(0, count, one_turn, 0)
    if keep:
        for t in range(count):
            for b in range(flow):
                rows = lax.broadcasted_iota(jnp.int32, (block, width), 0).astype(F32) + float(b * block)
                s.give[b * block:(b + 1) * block, t * width:(t + 1) * width] = jnp.where(
                    rows == s.along[t:t + 1, :], 1.0, 0.0).astype(BF16)

    def take_rows(t0):
        if keep:
            return s.take[t0 * width:(t0 + group) * width, :]
        cell = s.take[t0:t0 + group].reshape(group * width, seg)
        lanes = lax.broadcasted_iota(jnp.int32, (group * width, seg), 1).astype(F32)
        return jnp.concatenate(
            [jnp.where(cell - float(k * seg) == lanes, 1.0, 0.0).astype(BF16) for k in range(cells // seg)], axis=1)

    def give_rows(t0, b):
        if keep:
            return s.give[b * block:(b + 1) * block, t0 * width:(t0 + group) * width]
        rows = lax.broadcasted_iota(jnp.int32, (block, width), 0).astype(F32) + float(b * block)
        return jnp.concatenate(
            [jnp.where(rows == s.along[t:t + 1, :], 1.0, 0.0).astype(BF16) for t in range(t0, t0 + group)], axis=1)

    take_in(1)

    side_marks = [empty] * packs
    for b in range(flow):
        c = s.plane[0, b]
        side_marks = packed(side_marks, c, side_place(b))
        hi, lo = split(c)
        s.base[b * block:(b + 1) * block, 0:seg] = hi
        s.base[b * block:(b + 1) * block, seg:2 * seg] = lo
    for p in range(packs):
        s.side_out[p] = side_marks[p]
    start(side_copy, 0, in_span)

    def chunk(ref, t):
        return ref[:, :, t * seg:(t + 1) * seg].reshape(width, seg)

    def constants(i, carry):
        own_core = jnp.logical_and(i >= 2, i <= half)
        hop = jnp.where(i < 2, 0, jnp.where(i <= half, i - 1, i - half))
        from_me = lax.rem(me + flow - 2 * hop, flow)
        from_mate = lax.rem(mate + flow - 2 * hop, flow)
        f = jnp.where(jnp.logical_or(i == 0, own_core), from_me, from_mate)

        @pl.when(i == 1)
        def _():
            to_mate(2).wait_recv()

        @pl.when(own_core)
        def _():
            hand_on(2, hop)

        @pl.when(i > half)
        def _():
            relay(2, hop).wait_recv()

        @pl.when(own_core)
        def _():
            relay(2, hop).wait_send()

        k = jnp.concatenate([s.gain[f, :, t * seg:(t + 1) * seg] for t in range(count)], axis=0)
        k1 = k.astype(BF16)
        rest = k - k1.astype(F32)
        k2 = rest.astype(BF16)
        k3 = (rest - k2.astype(F32)).astype(BF16)
        sums = jnp.dot(jnp.concatenate([k1, k2, k3], axis=1), spread, preferred_element_type=F32)
        run = jnp.ones((channels, seg), F32)
        for t in range(count):
            rows = slice(t * channels, (t + 1) * channels)
            cols = slice(t * seg, (t + 1) * seg)
            kt, depth = k[rows], sums[rows, 0:seg]
            fore, rear = jnp.exp(-sums[rows, seg:2 * seg]), jnp.exp(-sums[rows, 2 * seg:])
            s.gain[f, :, cols] = (1.0 - jnp.exp(-kt)) * jnp.exp(depth)
            s.fall[f, :, cols] = jnp.exp(-depth)
            s.heat_of[f, :, cols] = (jnp.exp(kt) - 1.0) * capacity
            s.fore[f, :, cols] = fore
            s.rear[f, :, cols] = rear
            s.reach[f, :, cols] = fore * run
            run = run * (fore * rear)
        s.whole[f] = run
        return carry

    lax.fori_loop(0, flow, constants, 0)

    def march(run, first_t, last_t):
        base = s.base[...]
        for t0 in range(first_t, last_t, group):
            found = jnp.dot(take_rows(t0), base, preferred_element_type=F32)
            w = found[:, :seg] + found[:, seg:]
            gains = jnp.concatenate([chunk(s.gain, t) for t in range(t0, t0 + group)], axis=0)
            hi, lo = split(gains * w)
            sums = jnp.dot(jnp.concatenate([hi, lo], axis=1), s.tri[...], preferred_element_type=F32)
            for i in range(group):
                t = t0 + i
                rows = slice(i * width, (i + 1) * width)
                s.wall[t] = w[rows]
                into = chunk(s.fore, t) * run
                s.part[t] = sums[rows, :seg] + into
                run = chunk(s.rear, t) * (sums[rows, seg:] + into)
        return run

    def carries(run):
        enter = inlet
        for f in range(flow):
            s.enter[f] = enter
            enter = run[f * channels:(f + 1) * channels] + s.whole[f] * enter

    def heats(first_t, last_t):
        enter = s.enter[...].reshape(width, seg)
        for t in range(first_t, last_t):
            cool = chunk(s.fall, t) * (s.part[t] + chunk(s.reach, t) * enter)
            hi, lo = split(chunk(s.heat_of, t) * (s.wall[t] - cool))
            s.heat[t * width:(t + 1) * width, 0:seg] = hi
            s.heat[t * width:(t + 1) * width, seg:2 * seg] = lo

    def sinks(b, first_t, last_t):
        if keep:
            cols = slice(first_t * width, last_t * width)
            total = jnp.dot(s.give[:, cols] if b is None else s.give[b * block:(b + 1) * block, cols],
                            s.heat[cols, :], preferred_element_type=F32)
        else:
            total = jnp.zeros((block, 2 * seg), F32)
            for t0 in range(first_t, last_t, group):
                total = total + jnp.dot(give_rows(t0, b), s.heat[t0 * width:(t0 + group) * width, :],
                                        preferred_element_type=F32)
        return total[:, :seg] + total[:, seg:]

    def all_sinks(first_t, last_t):
        if keep:
            return sinks(None, first_t, last_t)
        return jnp.concatenate([sinks(b, first_t, last_t) for b in range(flow)], axis=0)

    def await_part(part, slot):
        arrived(row_copy(part), slot, in_flow)
        sent(row_copy(part), slot, in_flow)
        arrived(col_copy(part), slot, in_span)
        sent(col_copy(part), slot, in_span)

    def conduct(part, slot, later):
        marks = [empty] * col_packs
        halos = [merged(s.col_in[slot, part, 0, p], s.col_in[slot, part, 1, p]) for p in range(col_packs)]
        for z in members(part):
            c = s.field[slot, z]
            beside = around(c, s.row_in[slot, 0, z:z + 1, :], s.row_in[slot, 1, z:z + 1, :],
                            unpacked(halos, col_place(z)))
            under = s.plane[slot, me] if z == 1 else s.field[slot, z - 1]
            beside = beside + under + s.field[slot, z + 1]
            new = c + KAPPA * (beside - 6.0 * c) + gen_ref[z]
            s.field[later, z] = new
            note_rows(z, new)
            marks = packed(marks, new, col_place(z))
        for p in range(col_packs):
            s.col_out[part, p] = marks[p]

    def step(turn, carry):
        slot, later = lax.rem(turn, 2), lax.rem(turn + 1, 2)
        held, next_held = lax.rem(turn, 4), lax.rem(turn + 1, 4)
        more = turn < STEPS - 1

        await_part(0, slot)
        run = march(jnp.zeros((width, seg), F32), 0, count // 2)
        conduct(0, slot, later)

        @pl.when(turn > 0)
        def _():
            for hop in range(1, half):
                one_direct(held, hop).wait_send()
            one_to_mate(held).wait_send()

        @pl.when(turn > 1)
        def _():
            for hop in range(1, half):
                one_relay(held, hop).wait_send()
        s.one[next_held, me] = s.field[later, 1]

        @pl.when(more)
        def _():
            send_part(0, later)
            for hop in range(1, half):
                one_direct(next_held, hop).start()
            one_to_mate(next_held).start()
        await_part(1, slot)
        run = march(run, count // 2, count)
        conduct(1, slot, later)

        @pl.when(turn > 0)
        def _():
            for hop in range(1, half):
                one_direct(held, hop).wait_recv()
                one_relay(held, hop).start()

        @pl.when(turn == 0)
        def _():
            pass_on(3)
            pass_on(4)

        @pl.when(more)
        def _():
            send_part(1, later)
        await_part(2, slot)
        carries(run)
        heats(0, count // 2)
        conduct(2, slot, later)

        @pl.when(more)
        def _():
            send_part(2, later)
        await_part(3, slot)
        s.sink[...] = all_sinks(0, count // 2)
        heats(count // 2, count)
        conduct(3, slot, later)

        @pl.when(more)
        def _():
            send_part(3, later)

        @pl.when(turn == 0)
        def _():
            take_in(3)
            take_in(4)
            for hop in range(1, half):
                relay(1, hop).wait_send()
                relay(3, hop).wait_send()

        @pl.when(turn > 0)
        def _():
            one_to_mate(held).wait_recv()
            for hop in range(1, half):
                one_relay(held, hop).wait_recv()
        arrived(side_copy, slot, in_span)
        sent(side_copy, slot, in_span)
        halos = [merged(s.side_in[slot, 0, p], s.side_in[slot, 1, p]) for p in range(packs)]
        side_marks = [empty] * packs
        rest = all_sinks(count // 2, count)
        for b in range(flow):
            rows = slice(b * block, (b + 1) * block)
            c = s.plane[slot, b]
            low = s.plane[slot, b - 1, block - 1:block, :] if b else jnp.zeros((1, seg), F32)
            high = s.plane[slot, b + 1, 0:1, :] if b < flow - 1 else jnp.zeros((1, seg), F32)
            beside = around(c, low, high, unpacked(halos, side_place(b))) + s.one[held, b]
            new = c + KAPPA * (beside - 6.0 * c) + s.gen0[b] - (s.sink[rows, :] + rest[rows])
            s.plane[later, b] = new
            side_marks = packed(side_marks, new, side_place(b))
            hi, lo = split(new)
            s.base[b * block:(b + 1) * block, 0:seg] = hi
            s.base[b * block:(b + 1) * block, seg:2 * seg] = lo
        for p in range(packs):
            s.side_out[p] = side_marks[p]

        @pl.when(more)
        def _():
            start(side_copy, later, in_span)
        return carry

    lax.fori_loop(0, STEPS, step, 0)
    for kind in range(len(kinds)):
        for hop in range(1, half):
            direct(kind, hop).wait_send()
            if kind in (0, 4):
                relay(kind, hop).wait_send()
        to_mate(kind).wait_send()
    for hop in range(1, half):
        one_relay(0, hop).wait_send()
    last = STEPS % 2
    solid_out[0] = s.plane[last, me]
    for z in range(1, layers):
        solid_out[z] = s.field[last, z]
    rows = pl.ds(pl.multiple_of(me * channels, channels), channels)
    for t in range(count):
        cols = slice(t * seg, (t + 1) * seg)
        cool_out[:, cols] = s.fall[me, :, cols] * (s.part[t, rows, :] + s.reach[me, :, cols] * s.enter[me])


class Scratch:
    pass


def body(solid_start, heat_gen, conductance, heat_capacity, inlet_temp, wall_owner, wall_row):
    flow = lax.axis_size("flow")
    span = lax.axis_size("span")
    layers, block, seg = solid_start.shape
    channels, stations = conductance.shape
    count = stations // seg
    segs = channels * count
    width = flow * channels
    total = count * width
    cells = flow * block
    half = flow // 2
    lines = cells // 8
    keep = cells * total * 4 <= (8 << 20)
    group = max(1, 512 // width)
    packs = -(-lines // (seg // 2))
    col_packs = -(-(block // 8) // (seg // 2 // (layers // PARTS)))
    dims = (flow, span, layers, block, seg, channels, count, group, keep)
    vm = pltpu.VMEM
    dma = pltpu.SemaphoreType.DMA
    march = vm((flow, channels, stations), F32)
    parts = vm((count, width, seg), F32)
    scratch = dict(
        idx_own=vm((8, seg), F32), idx=vm((flow, 8, seg), F32),
        gen0=vm((flow, block, seg), F32), one=vm((4, flow, block, seg), F32),
        plane=vm((2, flow, block, seg), F32), field=vm((2, layers + 1, block, seg), F32),
        side_out=vm((packs, 8, seg), F32), side_in=vm((2, 2, packs, 8, seg), F32),
        sink=vm((cells, seg), F32),
        col_out=vm((PARTS, col_packs, 8, seg), F32), col_in=vm((2, PARTS, 2, col_packs, 8, seg), F32),
        row_out=vm((2, layers, seg), F32), row_in=vm((2, 2, layers, seg), F32),
        tri=vm((2 * seg, 2 * seg), BF16), seats=vm((flow, channels, 2 * seg), BF16),
        along=vm((count, width), F32),
        take=vm((total, cells), BF16) if keep else parts,
        base=vm((cells, 2 * seg), BF16), heat=vm((total, 2 * seg), BF16),
        gain=march, fall=march, heat_of=march, fore=march, rear=march, reach=march,
        whole=vm((flow, channels, seg), F32), enter=vm((flow, channels, seg), F32),
        wall=parts, part=parts,
        once_send=dma((5, flow - 1)), once_recv=dma((5, flow - 1)),
        one_send=dma((flow - 1,)), one_recv=dma((4, flow - 1)),
        side_send=dma((2,)), side_recv=dma((2, 2)),
        col_send=dma((PARTS, 2)), col_recv=dma((2, PARTS, 2)),
        row_send=dma((PARTS, 2)), row_recv=dma((2, PARTS, 2)),
    )
    if keep:
        scratch["give"] = vm((cells, total), BF16)
    names = list(scratch)

    def run(*refs):
        held = Scratch()
        for name, ref in zip(names, refs[9:]):
            setattr(held, name, ref)
        kernel(dims, *refs[:9], held)

    return pl.pallas_call(
        run,
        out_shape=(jax.ShapeDtypeStruct(solid_start.shape, F32),
                   jax.ShapeDtypeStruct(conductance.shape, F32)),
        in_specs=[pl.BlockSpec(memory_space=pltpu.VMEM)] * 7,
        out_specs=(pl.BlockSpec(memory_space=pltpu.VMEM),) * 2,
        scratch_shapes=list(scratch.values()),
        compiler_params=pltpu.CompilerParams(
            collective_id=0, has_side_effects=True, vmem_limit_bytes=63 << 20),
    )(wall_owner.reshape(segs // seg, seg), wall_row.reshape(segs // seg, seg),
      heat_capacity.reshape(1, channels), inlet_temp.reshape(1, channels),
      conductance, solid_start, heat_gen)


def solution(mesh):
    placed = (
        P(None, "flow", "span"),
        P(None, "flow", "span"),
        P("span", "flow"),
        P("span"),
        P("span"),
        P(("flow", "span"), None),
        P(("flow", "span"), None),
    )
    return jax.shard_map(
        body,
        mesh=mesh,
        in_specs=placed,
        out_specs=(P(None, "flow", "span"), P("span", "flow")),
        check_vma=False,
    )
```

```python
import jax
import jax.numpy as jnp
from jax import lax
from jax.experimental import pallas as pl
from jax.experimental.pallas import tpu as pltpu
from jax.sharding import PartitionSpec as P

STEPS = 10
PARTS = 4
KAPPA = 0.16
MESH = pl.DeviceIdType.MESH
F32 = jnp.float32
BF16 = jnp.bfloat16


def split(x):
    hi = x.astype(BF16)
    lo = (x - hi.astype(F32)).astype(BF16)
    return hi, lo


def kernel(dims, owner_ref, row_ref, cap_ref, inlet_ref, cond_ref, start_ref, gen_ref,
           solid_out, cool_out, s):
    flow, span, layers, block, seg, channels, count, group, keep = dims
    width = flow * channels
    cells = flow * block
    half = flow // 2
    tiles = block // 8
    lines = cells // 8
    packs = -(-lines // (seg // 2))
    deep = layers // PARTS
    me = lax.axis_index("flow")
    at = lax.axis_index("span")
    mate = me + 1 - 2 * lax.rem(me, 2)
    above, below = at > 0, at < span - 1
    before, after = me > 0, me < flow - 1

    lane = lax.broadcasted_iota(jnp.int32, (8, seg), 1)
    pair = lane // 2
    lane_b = lax.broadcasted_iota(jnp.int32, (block, seg), 1)
    row_b = lax.broadcasted_iota(jnp.int32, (block, seg), 0)
    first_b, last_b = lane_b == 0, lane_b == seg - 1
    top_b, low_b = row_b == 0, row_b == block - 1

    def remote(src, dst, send, recv, device):
        return pltpu.make_async_remote_copy(
            src_ref=src, dst_ref=dst, send_sem=send, recv_sem=recv,
            device_id=device, device_id_type=MESH)

    kinds = (
        (s.idx_own, lambda f: s.idx.at[f]),
        (start_ref.at[0], lambda f: s.plane.at[0, f]),
        (cond_ref, lambda f: s.gain.at[f]),
        (start_ref.at[1], lambda f: s.one.at[0, f]),
        (gen_ref.at[0], lambda f: s.gen0.at[f]),
    )

    def direct(kind, hop):
        src, dst = kinds[kind]
        to = lax.rem(me + 2 * hop, flow)
        return remote(src, dst(me), s.once_send.at[kind, 2 * hop - 1], s.once_recv.at[kind, 2 * hop - 1], (to, at))

    def to_mate(kind):
        src, dst = kinds[kind]
        return remote(src, dst(me), s.once_send.at[kind, 0], s.once_recv.at[kind, 0], (mate, at))

    def relay(kind, hop):
        _, dst = kinds[kind]
        origin = lax.rem(me + flow - 2 * hop, flow)
        return remote(dst(origin), dst(origin), s.once_send.at[kind, 2 * hop], s.once_recv.at[kind, 2 * hop], (mate, at))

    def one_direct(slot, hop):
        to = lax.rem(me + 2 * hop, flow)
        return remote(s.one.at[slot, me], s.one.at[slot, me],
                      s.one_send.at[2 * hop - 1], s.one_recv.at[slot, 2 * hop - 1], (to, at))

    def one_to_mate(slot):
        return remote(s.one.at[slot, me], s.one.at[slot, me],
                      s.one_send.at[0], s.one_recv.at[slot, 0], (mate, at))

    def one_relay(slot, hop):
        origin = lax.rem(me + flow - 2 * hop, flow)
        return remote(s.one.at[slot, origin], s.one.at[slot, origin],
                      s.one_send.at[2 * hop], s.one_recv.at[slot, 2 * hop], (mate, at))

    def side_copy(slot, side):
        return remote(s.side_out, s.side_in.at[slot, 1 - side],
                      s.side_send.at[side], s.side_recv.at[slot, 1 - side], (me, at - 1 + 2 * side))

    def col_copy(part):
        def copy(slot, side):
            return remote(s.col_out.at[part], s.col_in.at[slot, part, 1 - side],
                          s.col_send.at[part, side], s.col_recv.at[slot, part, 1 - side], (me, at - 1 + 2 * side))
        return copy

    def row_copy(part):
        rows = pl.ds(part * deep, deep)

        def copy(slot, side):
            return remote(s.row_out.at[side, rows], s.row_in.at[slot, 1 - side, rows],
                          s.row_send.at[part, side], s.row_recv.at[slot, part, 1 - side], (me - 1 + 2 * side, at))
        return copy

    def both(copy, pair_of, act):
        for side, there in enumerate(pair_of):
            @pl.when(there)
            def _():
                act(copy, side)

    in_span, in_flow = (above, below), (before, after)

    def start(copy, slot, pair_of):
        both(copy, pair_of, lambda c, side: c(slot, side).start())

    def sent(copy, slot, pair_of):
        both(copy, pair_of, lambda c, side: c(slot, side).wait_send())

    def arrived(copy, slot, pair_of):
        both(copy, pair_of, lambda c, side: c(slot, 1 - side).wait_recv())

    s.side_in[...] = jnp.zeros_like(s.side_in)
    s.col_in[...] = jnp.zeros_like(s.col_in)
    s.row_in[...] = jnp.zeros_like(s.row_in)
    s.idx_own[...] = jnp.zeros_like(s.idx_own)
    per = owner_ref.shape[0]
    s.idx_own[0:per, :] = owner_ref[...].astype(F32)
    s.idx_own[per:2 * per, :] = row_ref[...].astype(F32)
    barrier = pltpu.get_barrier_semaphore()
    for hop in range(1, flow):
        pl.semaphore_signal(barrier, inc=1, device_id=(lax.rem(me + hop, flow), at), device_id_type=MESH)
    for side, there in enumerate(in_span):
        @pl.when(there)
        def _():
            pl.semaphore_signal(barrier, inc=1, device_id=(me, at - 1 + 2 * side), device_id_type=MESH)
    pl.semaphore_wait(barrier, flow - 1 + above.astype(jnp.int32) + below.astype(jnp.int32))
    for kind in range(len(kinds)):
        for hop in range(1, half):
            direct(kind, hop).start()
        to_mate(kind).start()
    s.idx[me] = s.idx_own[...]
    s.plane[0, me] = start_ref[0]
    s.one[0, me] = start_ref[1]
    s.gain[me] = cond_ref[...]
    s.gen0[me] = gen_ref[0]

    def packed(marks, value, place):
        for r in range(tiles):
            p, k = place(r)
            turned = pltpu.roll(value[8 * r:8 * r + 8], 2 * k + 1, 1)
            marks[p] = jnp.where(pair == k, turned, marks[p])
        return marks

    def merged(low, high):
        return jnp.where(lax.rem(lane, 2) == 0, pltpu.roll(high, seg - 1, 1), pltpu.roll(low, 1, 1))

    def unpacked(marks, place):
        return jnp.concatenate(
            [pltpu.roll(marks[p], seg - 1 - 2 * k, 1) for p, k in (place(r) for r in range(tiles))], axis=0)

    def col_place(z):
        per_pack = seg // 2 // deep
        return lambda r: (r // per_pack, z % deep + deep * (r % per_pack))

    def side_place(b):
        return lambda r: divmod(b * tiles + r, seg // 2)

    col_packs = s.col_out.shape[1]
    empty = jnp.zeros((8, seg), F32)

    def around(c, low_row, high_row, halo):
        beside = jnp.where(top_b, low_row, pltpu.roll(c, 1, 0))
        beside = beside + jnp.where(low_b, high_row, pltpu.roll(c, block - 1, 0))
        beside = beside + jnp.where(first_b, halo, pltpu.roll(c, 1, 1))
        return beside + jnp.where(last_b, halo, pltpu.roll(c, seg - 1, 1))

    for side in range(2):
        s.row_out[side] = jnp.zeros_like(s.row_out[side])
    s.field[0, layers] = jnp.zeros((block, seg), F32)
    s.field[1, layers] = jnp.zeros((block, seg), F32)

    def note_rows(z, new):
        s.row_out[0, z:z + 1, :] = new[0:1, :]
        s.row_out[1, z:z + 1, :] = new[block - 1:block, :]

    def members(part):
        return range(max(1, part * deep), (part + 1) * deep)

    def send_part(part, slot):
        start(row_copy(part), slot, in_flow)
        start(col_copy(part), slot, in_span)

    for part in range(PARTS):
        marks = [empty] * col_packs
        for z in members(part):
            new = start_ref[z]
            s.field[0, z] = new
            note_rows(z, new)
            marks = packed(marks, new, col_place(z))
        for p in range(col_packs):
            s.col_out[part, p] = marks[p]
        send_part(part, 0)

    mid = seg // 2 - 1
    i2 = lax.rem(lax.broadcasted_iota(jnp.int32, (2 * seg, 2 * seg), 0), seg)
    j2 = lax.broadcasted_iota(jnp.int32, (2 * seg, 2 * seg), 1)
    tri = jnp.where((i2 <= j2) | (j2 >= seg), 1.0, 0.0).astype(BF16)
    s.tri[...] = tri
    i3 = lax.rem(lax.broadcasted_iota(jnp.int32, (3 * seg, 3 * seg), 0), seg)
    j3 = lax.broadcasted_iota(jnp.int32, (3 * seg, 3 * seg), 1)
    lower = jnp.where(i3 <= mid, 1.0, 0.0)
    spread = jnp.where(j3 < seg, jnp.where(i3 <= j3, 1.0, 0.0) - lower,
                       jnp.where(j3 < 2 * seg, lower, 1.0 - lower)).astype(BF16)
    eye = (lax.broadcasted_iota(jnp.int32, (channels, channels), 0)
           == lax.broadcasted_iota(jnp.int32, (channels, channels), 1))

    def column(ref):
        wide = jnp.where(eye, jnp.broadcast_to(ref[...], (channels, channels)), 0.0)
        return jnp.broadcast_to(jnp.sum(wide, axis=1, keepdims=True), (channels, seg))

    capacity, inlet = column(cap_ref), column(inlet_ref)

    def hand_on(kind, hop):
        direct(kind, hop).wait_recv()
        relay(kind, hop).start()

    def pass_on(kind):
        for hop in range(1, half):
            hand_on(kind, hop)

    def take_in(kind):
        to_mate(kind).wait_recv()
        for hop in range(1, half):
            relay(kind, hop).wait_recv()

    pass_on(0)
    pass_on(1)
    take_in(0)
    share = seg // count
    lane_i = lax.broadcasted_iota(jnp.int32, (channels, seg), 1) // count
    chan_i = lax.rem(lax.broadcasted_iota(jnp.int32, (channels, seg), 0), share)
    here = lane_i == chan_i

    def one_source(f, carry):
        def taken(base):
            rows = jnp.concatenate(
                [jnp.broadcast_to(s.idx[f, base + a:base + a + 1, :], (share, seg)) for a in range(per)], axis=0)
            return jnp.where(here, rows, 0.0).astype(BF16)
        s.seats[f] = jnp.concatenate([taken(0), taken(per)], axis=1)
        return carry

    lax.fori_loop(0, flow, one_source, 0)
    seats = s.seats[...].reshape(width, 2 * seg)
    ci = lax.broadcasted_iota(jnp.int32, (2 * seg, seg), 0)
    weight = jnp.where(ci < seg, float(block), 1.0)
    turn_of = lax.rem(ci, count)
    ri = lax.broadcasted_iota(jnp.int32, (count, 2 * seg), 1)
    rt = lax.broadcasted_iota(jnp.int32, (count, 2 * seg), 0)
    pick = jnp.where(lax.rem(ri, count) == rt, jnp.where(ri < seg, float(block), 1.0), 0.0).astype(BF16)
    s.along[...] = lax.dot_general(pick, seats, (((1,), (1,)), ((), ())), preferred_element_type=F32)

    def one_turn(t, carry):
        chosen = jnp.where(turn_of == t, weight, 0.0).astype(BF16)
        cell = jnp.dot(seats, chosen, preferred_element_type=F32)
        if keep:
            lanes = lax.broadcasted_iota(jnp.int32, (width, seg), 1).astype(F32)
            rows = pl.ds(pl.multiple_of(t * width, width), width)
            for k in range(cells // seg):
                s.take[rows, k * seg:(k + 1) * seg] = jnp.where(cell - float(k * seg) == lanes, 1.0, 0.0).astype(BF16)
        else:
            s.take[t] = cell
        return carry

    lax.fori_loop(0, count, one_turn, 0)
    if keep:
        for t in range(count):
            for b in range(flow):
                rows = lax.broadcasted_iota(jnp.int32, (block, width), 0).astype(F32) + float(b * block)
                s.give[b * block:(b + 1) * block, t * width:(t + 1) * width] = jnp.where(
                    rows == s.along[t:t + 1, :], 1.0, 0.0).astype(BF16)

    def take_rows(t0):
        if keep:
            return s.take[t0 * width:(t0 + group) * width, :]
        cell = s.take[t0:t0 + group].reshape(group * width, seg)
        lanes = lax.broadcasted_iota(jnp.int32, (group * width, seg), 1).astype(F32)
        return jnp.concatenate(
            [jnp.where(cell - float(k * seg) == lanes, 1.0, 0.0).astype(BF16) for k in range(cells // seg)], axis=1)

    def give_rows(t0, b):
        if keep:
            return s.give[b * block:(b + 1) * block, t0 * width:(t0 + group) * width]
        rows = lax.broadcasted_iota(jnp.int32, (block, width), 0).astype(F32) + float(b * block)
        return jnp.concatenate(
            [jnp.where(rows == s.along[t:t + 1, :], 1.0, 0.0).astype(BF16) for t in range(t0, t0 + group)], axis=1)

    take_in(1)

    side_marks = [empty] * packs
    for b in range(flow):
        c = s.plane[0, b]
        side_marks = packed(side_marks, c, side_place(b))
        hi, lo = split(c)
        s.base[b * block:(b + 1) * block, 0:seg] = hi
        s.base[b * block:(b + 1) * block, seg:2 * seg] = lo
    for p in range(packs):
        s.side_out[p] = side_marks[p]
    start(side_copy, 0, in_span)

    def chunk(ref, t):
        return ref[:, :, t * seg:(t + 1) * seg].reshape(width, seg)

    def constants(i, carry):
        own_core = jnp.logical_and(i >= 2, i <= half)
        hop = jnp.where(i < 2, 0, jnp.where(i <= half, i - 1, i - half))
        from_me = lax.rem(me + flow - 2 * hop, flow)
        from_mate = lax.rem(mate + flow - 2 * hop, flow)
        f = jnp.where(jnp.logical_or(i == 0, own_core), from_me, from_mate)

        @pl.when(i == 1)
        def _():
            to_mate(2).wait_recv()

        @pl.when(own_core)
        def _():
            hand_on(2, hop)

        @pl.when(i > half)
        def _():
            relay(2, hop).wait_recv()

        @pl.when(own_core)
        def _():
            relay(2, hop).wait_send()

        k = jnp.concatenate([s.gain[f, :, t * seg:(t + 1) * seg] for t in range(count)], axis=0)
        k1 = k.astype(BF16)
        rest = k - k1.astype(F32)
        k2 = rest.astype(BF16)
        k3 = (rest - k2.astype(F32)).astype(BF16)
        sums = jnp.dot(jnp.concatenate([k1, k2, k3], axis=1), spread, preferred_element_type=F32)
        run = jnp.ones((channels, seg), F32)
        for t in range(count):
            rows = slice(t * channels, (t + 1) * channels)
            cols = slice(t * seg, (t + 1) * seg)
            kt, depth = k[rows], sums[rows, 0:seg]
            fore, rear = jnp.exp(-sums[rows, seg:2 * seg]), jnp.exp(-sums[rows, 2 * seg:])
            s.gain[f, :, cols] = (1.0 - jnp.exp(-kt)) * jnp.exp(depth)
            s.fall[f, :, cols] = jnp.exp(-depth)
            s.heat_of[f, :, cols] = (jnp.exp(kt) - 1.0) * capacity
            s.fore[f, :, cols] = fore
            s.rear[f, :, cols] = rear
            s.reach[f, :, cols] = fore * run
            run = run * (fore * rear)
        s.whole[f] = run
        return carry

    lax.fori_loop(0, flow, constants, 0)

    def march(run, first_t, last_t):
        base = s.base[...]
        for t0 in range(first_t, last_t, group):
            found = jnp.dot(take_rows(t0), base, preferred_element_type=F32)
            w = found[:, :seg] + found[:, seg:]
            gains = jnp.concatenate([chunk(s.gain, t) for t in range(t0, t0 + group)], axis=0)
            hi, lo = split(gains * w)
            sums = jnp.dot(jnp.concatenate([hi, lo], axis=1), s.tri[...], preferred_element_type=F32)
            for i in range(group):
                t = t0 + i
                rows = slice(i * width, (i + 1) * width)
                s.wall[t] = w[rows]
                into = chunk(s.fore, t) * run
                s.part[t] = sums[rows, :seg] + into
                run = chunk(s.rear, t) * (sums[rows, seg:] + into)
        return run

    def carries(run):
        enter = inlet
        for f in range(flow):
            s.enter[f] = enter
            enter = run[f * channels:(f + 1) * channels] + s.whole[f] * enter

    def heats(first_t, last_t):
        enter = s.enter[...].reshape(width, seg)
        for t in range(first_t, last_t):
            cool = chunk(s.fall, t) * (s.part[t] + chunk(s.reach, t) * enter)
            hi, lo = split(chunk(s.heat_of, t) * (s.wall[t] - cool))
            s.heat[t * width:(t + 1) * width, 0:seg] = hi
            s.heat[t * width:(t + 1) * width, seg:2 * seg] = lo

    def sinks(b, first_t, last_t):
        if keep:
            cols = slice(first_t * width, last_t * width)
            total = jnp.dot(s.give[:, cols] if b is None else s.give[b * block:(b + 1) * block, cols],
                            s.heat[cols, :], preferred_element_type=F32)
        else:
            total = jnp.zeros((block, 2 * seg), F32)
            for t0 in range(first_t, last_t, group):
                total = total + jnp.dot(give_rows(t0, b), s.heat[t0 * width:(t0 + group) * width, :],
                                        preferred_element_type=F32)
        return total[:, :seg] + total[:, seg:]

    def all_sinks(first_t, last_t):
        if keep:
            return sinks(None, first_t, last_t)
        return jnp.concatenate([sinks(b, first_t, last_t) for b in range(flow)], axis=0)

    def await_part(part, slot):
        arrived(row_copy(part), slot, in_flow)
        sent(row_copy(part), slot, in_flow)
        arrived(col_copy(part), slot, in_span)
        sent(col_copy(part), slot, in_span)

    def conduct(part, slot, later):
        marks = [empty] * col_packs
        halos = [merged(s.col_in[slot, part, 0, p], s.col_in[slot, part, 1, p]) for p in range(col_packs)]
        for z in members(part):
            c = s.field[slot, z]
            beside = around(c, s.row_in[slot, 0, z:z + 1, :], s.row_in[slot, 1, z:z + 1, :],
                            unpacked(halos, col_place(z)))
            under = s.plane[slot, me] if z == 1 else s.field[slot, z - 1]
            beside = beside + under + s.field[slot, z + 1]
            new = c + KAPPA * (beside - 6.0 * c) + gen_ref[z]
            s.field[later, z] = new
            note_rows(z, new)
            marks = packed(marks, new, col_place(z))
        for p in range(col_packs):
            s.col_out[part, p] = marks[p]

    def step(turn, carry):
        slot, later = lax.rem(turn, 2), lax.rem(turn + 1, 2)
        held, next_held = lax.rem(turn, 4), lax.rem(turn + 1, 4)
        more = turn < STEPS - 1

        await_part(0, slot)
        run = march(jnp.zeros((width, seg), F32), 0, count // 2)
        conduct(0, slot, later)

        @pl.when(turn > 0)
        def _():
            for hop in range(1, half):
                one_direct(held, hop).wait_send()
            one_to_mate(held).wait_send()

        @pl.when(turn > 1)
        def _():
            for hop in range(1, half):
                one_relay(held, hop).wait_send()
        s.one[next_held, me] = s.field[later, 1]

        @pl.when(more)
        def _():
            send_part(0, later)
            for hop in range(1, half):
                one_direct(next_held, hop).start()
            one_to_mate(next_held).start()
        await_part(1, slot)
        run = march(run, count // 2, count)
        conduct(1, slot, later)

        @pl.when(turn > 0)
        def _():
            for hop in range(1, half):
                one_direct(held, hop).wait_recv()
                one_relay(held, hop).start()

        @pl.when(turn == 0)
        def _():
            pass_on(3)
            pass_on(4)

        @pl.when(more)
        def _():
            send_part(1, later)
        await_part(2, slot)
        carries(run)
        heats(0, count // 2)
        conduct(2, slot, later)

        @pl.when(more)
        def _():
            send_part(2, later)
        await_part(3, slot)
        s.sink[...] = all_sinks(0, count // 2)
        heats(count // 2, count)
        conduct(3, slot, later)

        @pl.when(more)
        def _():
            send_part(3, later)

        @pl.when(turn == 0)
        def _():
            take_in(3)
            take_in(4)
            for hop in range(1, half):
                relay(1, hop).wait_send()
                relay(3, hop).wait_send()

        @pl.when(turn > 0)
        def _():
            one_to_mate(held).wait_recv()
            for hop in range(1, half):
                one_relay(held, hop).wait_recv()
        arrived(side_copy, slot, in_span)
        sent(side_copy, slot, in_span)
        halos = [merged(s.side_in[slot, 0, p], s.side_in[slot, 1, p]) for p in range(packs)]
        side_marks = [empty] * packs
        rest = all_sinks(count // 2, count)
        for b in range(flow):
            rows = slice(b * block, (b + 1) * block)
            c = s.plane[slot, b]
            low = s.plane[slot, b - 1, block - 1:block, :] if b else jnp.zeros((1, seg), F32)
            high = s.plane[slot, b + 1, 0:1, :] if b < flow - 1 else jnp.zeros((1, seg), F32)
            beside = around(c, low, high, unpacked(halos, side_place(b))) + s.one[held, b]
            new = c + KAPPA * (beside - 6.0 * c) + s.gen0[b] - (s.sink[rows, :] + rest[rows])
            s.plane[later, b] = new
            side_marks = packed(side_marks, new, side_place(b))
            hi, lo = split(new)
            s.base[b * block:(b + 1) * block, 0:seg] = hi
            s.base[b * block:(b + 1) * block, seg:2 * seg] = lo
        for p in range(packs):
            s.side_out[p] = side_marks[p]

        @pl.when(more)
        def _():
            start(side_copy, later, in_span)
        return carry

    lax.fori_loop(0, STEPS, step, 0)
    for kind in range(len(kinds)):
        for hop in range(1, half):
            direct(kind, hop).wait_send()
            if kind in (0, 4):
                relay(kind, hop).wait_send()
        to_mate(kind).wait_send()
    for hop in range(1, half):
        one_relay(0, hop).wait_send()
    last = STEPS % 2
    solid_out[0] = s.plane[last, me]
    for z in range(1, layers):
        solid_out[z] = s.field[last, z]
    rows = pl.ds(pl.multiple_of(me * channels, channels), channels)
    for t in range(count):
        cols = slice(t * seg, (t + 1) * seg)
        cool_out[:, cols] = s.fall[me, :, cols] * (s.part[t, rows, :] + s.reach[me, :, cols] * s.enter[me])


class Scratch:
    pass


def body(solid_start, heat_gen, conductance, heat_capacity, inlet_temp, wall_owner, wall_row):
    flow = lax.axis_size("flow")
    span = lax.axis_size("span")
    layers, block, seg = solid_start.shape
    channels, stations = conductance.shape
    count = stations // seg
    segs = channels * count
    width = flow * channels
    total = count * width
    cells = flow * block
    half = flow // 2
    lines = cells // 8
    keep = cells * total * 4 <= (8 << 20)
    group = max(1, 512 // width)
    packs = -(-lines // (seg // 2))
    col_packs = -(-(block // 8) // (seg // 2 // (layers // PARTS)))
    dims = (flow, span, layers, block, seg, channels, count, group, keep)
    vm = pltpu.VMEM
    dma = pltpu.SemaphoreType.DMA
    march = vm((flow, channels, stations), F32)
    parts = vm((count, width, seg), F32)
    scratch = dict(
        idx_own=vm((8, seg), F32), idx=vm((flow, 8, seg), F32),
        gen0=vm((flow, block, seg), F32), one=vm((4, flow, block, seg), F32),
        plane=vm((2, flow, block, seg), F32), field=vm((2, layers + 1, block, seg), F32),
        side_out=vm((packs, 8, seg), F32), side_in=vm((2, 2, packs, 8, seg), F32),
        sink=vm((cells, seg), F32),
        col_out=vm((PARTS, col_packs, 8, seg), F32), col_in=vm((2, PARTS, 2, col_packs, 8, seg), F32),
        row_out=vm((2, layers, seg), F32), row_in=vm((2, 2, layers, seg), F32),
        tri=vm((2 * seg, 2 * seg), BF16), seats=vm((flow, channels, 2 * seg), BF16),
        along=vm((count, width), F32),
        take=vm((total, cells), BF16) if keep else parts,
        base=vm((cells, 2 * seg), BF16), heat=vm((total, 2 * seg), BF16),
        gain=march, fall=march, heat_of=march, fore=march, rear=march, reach=march,
        whole=vm((flow, channels, seg), F32), enter=vm((flow, channels, seg), F32),
        wall=parts, part=parts,
        once_send=dma((5, flow - 1)), once_recv=dma((5, flow - 1)),
        one_send=dma((flow - 1,)), one_recv=dma((4, flow - 1)),
        side_send=dma((2,)), side_recv=dma((2, 2)),
        col_send=dma((PARTS, 2)), col_recv=dma((2, PARTS, 2)),
        row_send=dma((PARTS, 2)), row_recv=dma((2, PARTS, 2)),
    )
    if keep:
        scratch["give"] = vm((cells, total), BF16)
    names = list(scratch)

    def run(*refs):
        held = Scratch()
        for name, ref in zip(names, refs[9:]):
            setattr(held, name, ref)
        kernel(dims, *refs[:9], held)

    return pl.pallas_call(
        run,
        out_shape=tuple(
            vm(x.shape, F32) if keep else jax.ShapeDtypeStruct(x.shape, F32)
            for x in (solid_start, conductance)),
        in_specs=[pl.BlockSpec(memory_space=pltpu.VMEM)] * 7,
        out_specs=(pl.BlockSpec(memory_space=pltpu.VMEM),) * 2,
        scratch_shapes=list(scratch.values()),
        compiler_params=pltpu.CompilerParams(
            collective_id=0, has_side_effects=True, vmem_limit_bytes=(62 if keep else 63) << 20),
    )(wall_owner.reshape(segs // seg, seg), wall_row.reshape(segs // seg, seg),
      heat_capacity.reshape(1, channels), inlet_temp.reshape(1, channels),
      conductance, solid_start, heat_gen)


def solution(mesh):
    placed = (
        P(None, "flow", "span"),
        P(None, "flow", "span"),
        P("span", "flow"),
        P("span"),
        P("span"),
        P(("flow", "span"), None),
        P(("flow", "span"), None),
    )
    return jax.shard_map(
        body,
        mesh=mesh,
        in_specs=placed,
        out_specs=(P(None, "flow", "span"), P("span", "flow")),
        check_vma=False,
    )
```
